32 devices in a mesh: dp: 8 (over z, y), mp: 4 (over x, core).
Axes of the slice: x: 2, y: 2, z: 4, core: 2. Of those that a mesh axis runs over, the one named last changes fastest.
Arguments:
- prefix_hidden: bfloat16 [32, 1024, 2048], P(('dp', 'mp')), may hold values from -6 to 6
- prefix_len: int32 [32], P('dp'), may hold values from 256 to 1024
- actions: float32 [32, 50, 32], P('dp'), may hold values from -6 to 6
- noise: float32 [32, 50, 32], P('dp'), may hold values from -6 to 6
- time_index: int32 [32], P('dp'), may hold values from 0 to 999
- prefix_gain: float32 [2048], replicated, may hold values from 0.25 to 1.75
- key_weight: bfloat16 [2048, 256], P('dp'), may hold values from -0.125 to 0.125
- value_weight: bfloat16 [2048, 256], P('dp'), may hold values from -0.125 to 0.125
- action_in: bfloat16 [32, 1024], replicated, may hold values from -1 to 1
- attn_gain: float32 [1024], replicated, may hold values from 0.25 to 1.75
- query_w: bfloat16 [1024, 2048], P('dp', 'mp'), may hold values from -0.1875 to 0.1875
- akey_w: bfloat16 [1024, 256], P('dp'), may hold values from -0.1875 to 0.1875
- avalue_w: bfloat16 [1024, 256], P('dp'), may hold values from -0.1875 to 0.1875
- out_w: bfloat16 [2048, 1024], P('mp', 'dp'), may hold values from -0.125 to 0.125
- mlp_gain: float32 [1024], replicated, may hold values from 0.25 to 1.75
- gate_w: bfloat16 [1024, 4096], P('dp', 'mp'), may hold values from -0.1875 to 0.1875
- up_w: bfloat16 [1024, 4096], P('dp', 'mp'), may hold values from -0.1875 to 0.1875
- down_w: bfloat16 [4096, 1024], P('mp', 'dp'), may hold values from -0.09375 to 0.09375
- final_gain: float32 [1024], replicated, may hold values from 0.25 to 1.75
- head_w: bfloat16 [1024, 32], replicated, may hold values from -0.1875 to 0.1875
Outputs:
- velocity: float32 [32, 50, 32], P(('dp', 'mp'))
- ep_loss: float32 [32], P(('dp', 'mp'))
The draws below stay inside these ranges and needn't reach their ends.
Inputs may be any that keep to these rules, and one draw needn't show every extreme that they name: `prefix_len`: prefix positions at or above an episode's length are padding that no output reads.
All inputs are finite; a program needn't handle non-finite values.
Results may differ from the reference program's by a relative error of at most 0.009.
Values may be sent and summed in bfloat16 or wider, within the bound.
No kernel may reach another device: no remote copies, remote signals or barrier semaphores. Data moves between devices by JAX's collectives and lax.ppermute only.
A program may use at most 64 MiB of HBM per device.

```python
import math
import jax
import jax.numpy as jnp
from jax import lax

D = 2048
DE = 1024
HEADS = 8
HD = 256
FFE = 4096
ADIM = 32
SPAN = 50
PMAX = 1024
TSTEPS = 1000
EPIS = 32


def set_ends(drawn, rng, least, high):
    place = [jax.random.randint(jax.random.fold_in(rng, axis), (), 0, length) for axis, length in enumerate(drawn.shape)]
    widest = drawn.shape.index(max(drawn.shape))
    neighbour = place[:widest] + [(place[widest] + 1) % drawn.shape[widest]] + place[widest + 1:]
    return drawn.at[tuple(place)].set(least).at[tuple(neighbour)].set(high)


def block_levels(own_key, dims, pieces, smallest, top_value):
    factor_of, own = 1.0, jax.random.fold_in(own_key, 6)
    for position, shards_of in pieces:
        heights = jnp.exp(jax.random.uniform(jax.random.fold_in(own, position), (shards_of,), jnp.float32, smallest / len(pieces), top_value / len(pieces)))
        factor_of = factor_of * jnp.repeat(heights, dims[position] // shards_of).reshape([-1 if axis == position else 1 for axis in range(len(dims))])
    return factor_of


def normal_values(own_key, dims, deviation, bound, split=(), kind=jnp.bfloat16):
    drawn = jax.random.normal(own_key, dims, jnp.float32) * deviation
    if len(split) > 0:
        drawn = block_levels(own_key, dims, split, -0.22, 0.18) * drawn
    return jnp.clip(drawn, min=-bound, max=bound).astype(kind)


def setup_inputs(seed: int = 0) -> dict:
    key_of = jax.random.split(jax.random.key(seed), 21)
    prefix_hidden = normal_values(key_of[0], (EPIS, PMAX, D), 1.0, 6.0, ((0, 32),))
    prefix_len = set_ends(jax.random.randint(key_of[1], (EPIS,), PMAX // 4, PMAX + 1), jax.random.fold_in(key_of[1], 1), PMAX // 4, PMAX).astype(jnp.int32)
    actions = normal_values(key_of[2], (EPIS, SPAN, ADIM), 1.0, 6.0, ((0, 8),), jnp.float32)
    noise = normal_values(key_of[3], (EPIS, SPAN, ADIM), 1.0, 6.0, ((0, 8),), jnp.float32)
    time_index = set_ends(jax.random.randint(key_of[4], (EPIS,), 0, TSTEPS), jax.random.fold_in(key_of[4], 1), 0, TSTEPS - 1).astype(jnp.int32)
    prefix_gain = jnp.clip(1.0 + 0.15 * jax.random.normal(key_of[5], (D,), jnp.float32), 0.25, 1.75)
    key_weight = normal_values(key_of[6], (D, HD), D ** -0.5, 0.125, ((0, 8),))
    value_weight = normal_values(key_of[7], (D, HD), D ** -0.5, 0.125, ((0, 8),))
    action_in = normal_values(key_of[8], (ADIM, DE), ADIM ** -0.5, 1.0)
    attn_gain = jnp.clip(1.0 + 0.15 * jax.random.normal(key_of[9], (DE,), jnp.float32), 0.25, 1.75)
    query_w = normal_values(key_of[10], (DE, HEADS * HD), DE ** -0.5, 0.1875, ((0, 8), (1, 4)))
    akey_w = normal_values(key_of[11], (DE, HD), DE ** -0.5, 0.1875, ((0, 8),))
    avalue_w = normal_values(key_of[12], (DE, HD), DE ** -0.5, 0.1875, ((0, 8),))
    out_w = normal_values(key_of[13], (HEADS * HD, DE), (HEADS * HD) ** -0.5, 0.125, ((0, 4), (1, 8)))
    mlp_gain = jnp.clip(1.0 + 0.15 * jax.random.normal(key_of[14], (DE,), jnp.float32), 0.25, 1.75)
    gate_w = normal_values(key_of[15], (DE, FFE), DE ** -0.5, 0.1875, ((0, 8), (1, 4)))
    up_w = normal_values(key_of[16], (DE, FFE), DE ** -0.5, 0.1875, ((0, 8), (1, 4)))
    down_w = normal_values(key_of[17], (FFE, DE), FFE ** -0.5, 0.09375, ((0, 4), (1, 8)))
    final_gain = jnp.clip(1.0 + 0.15 * jax.random.normal(key_of[18], (DE,), jnp.float32), 0.25, 1.75)
    head_w = normal_values(key_of[19], (DE, ADIM), DE ** -0.5, 0.1875)
    return dict(prefix_hidden=prefix_hidden, prefix_len=prefix_len, actions=actions, noise=noise, time_index=time_index, prefix_gain=prefix_gain, key_weight=key_weight, value_weight=value_weight, action_in=action_in, attn_gain=attn_gain, query_w=query_w, akey_w=akey_w, avalue_w=avalue_w, out_w=out_w, mlp_gain=mlp_gain, gate_w=gate_w, up_w=up_w, down_w=down_w, final_gain=final_gain, head_w=head_w)


def rms(values, gain):
    return values * lax.rsqrt(lax.optimization_barrier(jnp.mean(values * values, axis=-1, keepdims=True)) + 1e-06) * gain

def time_embed(times, width):
    half = width // 2
    steps = jnp.arange(half, dtype=jnp.float32)
    period = 0.004 * jnp.power(jnp.float32(1000.0), steps / (half - 1))
    angle = times[:, None] * (2.0 * math.pi) / period[None, :]
    return jnp.concatenate([jnp.sin(angle), jnp.cos(angle)], axis=-1)

def reference(prefix_hidden, prefix_len, actions, noise, time_index, prefix_gain, key_weight, value_weight, action_in, attn_gain, query_w, akey_w, avalue_w, out_w, mlp_gain, gate_w, up_w, down_w, final_gain, head_w):
    times = (time_index.astype(jnp.float32) + 0.5) / TSTEPS
    x_t = times[:, None, None] * noise + (1.0 - times)[:, None, None] * actions
    target = noise - actions
    x_in = x_t.reshape(EPIS * SPAN, ADIM).astype(jnp.bfloat16)
    temb = time_embed(times, DE)
    h0 = jnp.dot(x_in, action_in, preferred_element_type=jnp.float32).reshape(EPIS, SPAN, DE) + temb[:, None, :]
    h0 = h0.reshape(EPIS * SPAN, DE)

    def project(hidden):
        normed = rms(hidden.astype(jnp.float32), prefix_gain).astype(jnp.bfloat16)
        keys = jnp.dot(normed, key_weight, preferred_element_type=jnp.float32).astype(jnp.bfloat16)
        vals = jnp.dot(normed, value_weight, preferred_element_type=jnp.float32).astype(jnp.bfloat16)
        return (keys, vals)
    prefix_keys, prefix_vals = lax.map(project, prefix_hidden)
    normed = rms(h0, attn_gain).astype(jnp.bfloat16)
    query = (jnp.dot(normed, query_w, preferred_element_type=jnp.float32) * HD ** (-0.5)).astype(jnp.bfloat16)
    query = query.reshape(EPIS, SPAN * HEADS, HD)
    akeys = jnp.dot(normed, akey_w, preferred_element_type=jnp.float32).astype(jnp.bfloat16).reshape(EPIS, SPAN, HD)
    avals = jnp.dot(normed, avalue_w, preferred_element_type=jnp.float32).astype(jnp.bfloat16).reshape(EPIS, SPAN, HD)

    def attend(items):
        rows, pkeys, pvals, keys_a, vals_a, length = items
        keys = jnp.concatenate([pkeys, keys_a], axis=0)
        vals = jnp.concatenate([pvals, vals_a], axis=0)
        live = jnp.concatenate([jnp.arange(PMAX, dtype=jnp.int32) < length, jnp.ones((SPAN,), dtype=bool)])
        scores = jnp.dot(rows, keys.T, preferred_element_type=jnp.float32)
        probs = jnp.where(live[None, :], jnp.exp(scores), 0.0)
        total = lax.optimization_barrier(jnp.sum(probs, axis=-1, keepdims=True))
        weighted = jnp.dot(probs.astype(jnp.bfloat16), vals, preferred_element_type=jnp.float32)
        return (weighted / total).astype(jnp.bfloat16)
    attn = lax.map(attend, (query, prefix_keys, prefix_vals, akeys, avals, prefix_len))
    attn = attn.reshape(EPIS * SPAN, HEADS * HD)
    h1 = h0 + jnp.dot(attn, out_w, preferred_element_type=jnp.float32)
    mixed = rms(h1, mlp_gain).astype(jnp.bfloat16)
    gate = jnp.dot(mixed, gate_w, preferred_element_type=jnp.float32)
    upper = jnp.dot(mixed, up_w, preferred_element_type=jnp.float32)
    hidden = (jax.nn.gelu(gate, approximate=True) * upper).astype(jnp.bfloat16)
    h2 = h1 + jnp.dot(hidden, down_w, preferred_element_type=jnp.float32)
    final = rms(h2, final_gain).astype(jnp.bfloat16)
    velocity = jnp.dot(final, head_w, preferred_element_type=jnp.float32).reshape(EPIS, SPAN, ADIM)
    diff = velocity - target
    ep_loss = lax.optimization_barrier(jnp.mean(diff * diff, axis=(1, 2)))
    return (velocity, ep_loss)
```

```python
import math

import jax
import jax.numpy as jnp
from jax import lax
from jax.experimental import pallas as pl
from jax.experimental.pallas import tpu as pltpu
from jax.sharding import Mesh
from jax.sharding import PartitionSpec as P

TSTEPS = 1000
BF = jnp.bfloat16
F32 = jnp.float32
LANES = 128


def rms(values, gain):
    return values * lax.rsqrt(jnp.mean(values * values, axis=-1, keepdims=True) + 1e-06) * gain


def time_embed(times, width):
    half = width // 2
    steps = jnp.arange(half, dtype=F32)
    period = 0.004 * jnp.power(F32(1000.0), steps / (half - 1))
    angle = times[:, None] * (2.0 * math.pi) / period[None, :]
    return jnp.concatenate([jnp.sin(angle), jnp.cos(angle)], axis=-1)


def dot(a, b):
    return jnp.dot(a, b, preferred_element_type=F32)


def blocks_of(values, index, per):
    rows, cols = values.shape
    count = cols // per
    if per % LANES:
        moved = jnp.take(values.reshape(rows, count, per), index, axis=1)
        return moved.reshape(rows, cols)

    def kernel(index_ref, values_ref, out_ref):
        for b in range(count):
            start = pl.multiple_of(index_ref[b] * per, per)
            out_ref[:, b * per : (b + 1) * per] = values_ref[:, pl.ds(start, per)]

    return pl.pallas_call(
        kernel,
        out_shape=jax.ShapeDtypeStruct(values.shape, values.dtype),
        in_specs=[
            pl.BlockSpec(memory_space=pltpu.SMEM),
            pl.BlockSpec(memory_space=pltpu.VMEM),
        ],
        out_specs=pl.BlockSpec(memory_space=pltpu.VMEM),
        name="column_blocks",
    )(index, values)


def normed_blocks(values, gain, index, per):
    rows, cols = values.shape
    count = cols // per
    if per % LANES:
        return blocks_of(rms(values.astype(F32), gain).astype(BF), index, per)
    step = math.gcd(rows, 256)

    def kernel(index_ref, values_ref, gain_ref, out_ref):
        v = values_ref[...].astype(F32)
        scale = lax.rsqrt(jnp.mean(v * v, axis=-1, keepdims=True) + 1e-06)
        for b in range(count):
            start = pl.multiple_of(index_ref[b] * per, per)
            part = values_ref[:, pl.ds(start, per)].astype(F32)
            part = part * scale * gain_ref[:, pl.ds(start, per)]
            out_ref[:, b * per : (b + 1) * per] = part.astype(BF)

    return pl.pallas_call(
        kernel,
        grid=(rows // step,),
        out_shape=jax.ShapeDtypeStruct(values.shape, BF),
        in_specs=[
            pl.BlockSpec(memory_space=pltpu.SMEM),
            pl.BlockSpec((step, cols), lambda s: (s, 0)),
            pl.BlockSpec((1, cols), lambda s: (0, 0)),
        ],
        out_specs=pl.BlockSpec((step, cols), lambda s: (s, 0)),
        name="normed_blocks",
    )(index, values, gain.reshape(1, cols))


def make(no, ni, nx, nc):
    def flip(value, axis):
        return lax.ppermute(value, axis, [(0, 1), (1, 0)])

    def cross(value, di, dx):
        pairs = [
            (i * nx + x, (i ^ di) * nx + (x ^ dx)) for i in range(ni) for x in range(nx)
        ]
        return lax.ppermute(value, ("i", "x"), pairs)

    RELS = ((0, 0), (1, 0), (0, 1), (1, 1))

    def spread(value):
        return [value] + [cross(value, di, dx) for di, dx in RELS[1:]]

    def exchange(parts):
        return [parts[0]] + [cross(p, di, dx) for p, (di, dx) in zip(parts[1:], RELS[1:])]

    def ring(value):
        if no <= 4:
            return [
                lax.ppermute(
                    value,
                    ("o", "i", "c"),
                    [
                        ((o * ni + i) * nc + c, (((o + r) % no) * ni + c) * nc + i)
                        for o in range(no)
                        for i in range(ni)
                        for c in range(nc)
                    ],
                )
                for r in range(no)
            ]
        value = lax.ppermute(
            value, ("i", "c"), [(i * nc + c, c * nc + i) for i in range(ni) for c in range(nc)]
        )
        whole = lax.all_gather(value, "o", axis=0, tiled=False)
        here = lax.axis_index("o")
        return [
            lax.dynamic_index_in_dim(whole, (here - r) % no, 0, keepdims=False) for r in range(no)
        ]

    def on_device(
        prefix_hidden,
        prefix_len,
        actions,
        noise,
        time_index,
        prefix_gain,
        key_weight,
        value_weight,
        action_in,
        attn_gain,
        query_w,
        akey_w,
        avalue_w,
        out_w,
        mlp_gain,
        gate_w,
        up_w,
        down_w,
        final_gain,
        head_w,
    ):
        own_eps, positions, width = prefix_hidden.shape
        group_eps, span, adim = actions.shape
        expert = action_in.shape[1]
        hd = key_weight.shape[1]
        oo, ii, xx, cc = (lax.axis_index(a) for a in ("o", "i", "x", "c"))
        member = xx * nc + cc

        def order(first, second, at):
            own_first = at == 0
            return jnp.where(own_first, first, second), jnp.where(own_first, second, first)

        own_kv = jnp.where(xx == 0, key_weight, value_weight)
        half = own_kv.shape[0] // nc
        own_kv = lax.dynamic_slice_in_dim(own_kv, cc * half, half, 0)
        akv = jnp.concatenate([akey_w, avalue_w], axis=1)
        quarter = akv.shape[1] // (nx * nc)
        akv = lax.dynamic_slice_in_dim(akv, member * quarter, quarter, 1)
        heads_cols = query_w.shape[1]
        qa_cols = heads_cols + quarter
        per = query_w.shape[0]
        fold = half // per if half % per == 0 else 0
        first = jnp.concatenate(
            [query_w, akv] + [own_kv[f * per : (f + 1) * per] for f in range(fold)], axis=1
        )
        got = ring(first)
        qa_own = jnp.concatenate([g[:, :qa_cols] for g in got], axis=0)
        kv_own = jnp.concatenate(
            [g[:, qa_cols + f * hd : qa_cols + (f + 1) * hd] for g in got for f in range(fold)],
            axis=0,
        )
        qa_oth = flip(qa_own, "c")
        kv_all = spread(kv_own)
        kv_same = jnp.concatenate([kv_all[0], kv_all[1]], axis=0)
        kv_diff = jnp.concatenate([kv_all[2], kv_all[3]], axis=0)
        kv_same_c, kv_diff_c = flip(kv_same, "c"), flip(kv_diff, "c")

        turn = (oo - jnp.arange(no, dtype=jnp.int32)) % no
        expert_index = jnp.concatenate([turn * nc + cc, turn * nc + (1 - cc)])
        prefix_index = jnp.concatenate(
            [
                (turn * ni + c) * nc + i
                for c in (cc, 1 - cc)
                for i in (ii, 1 - ii)
            ]
        )
        per_col = expert // (no * nc)

        times = (time_index.astype(F32) + 0.5) / TSTEPS
        x_t = times[:, None, None] * noise + (1.0 - times)[:, None, None] * actions
        x_in = x_t.astype(BF)
        per_eps = group_eps // (nx * nc)

        def mine_of(values):
            v = values.reshape((nx, nc, per_eps) + values.shape[1:])
            return lax.dynamic_index_in_dim(v, cc, 1, keepdims=False)

        packed = jnp.concatenate(
            [
                mine_of(x_in).astype(F32),
                jnp.broadcast_to(mine_of(times)[..., None, None], (nx, per_eps, 1, adim)),
            ],
            axis=2,
        )
        packed_oth = flip(packed, "i")
        a0, a1 = order(packed[0], packed[1], xx)
        b0, b1 = order(packed_oth[0], packed_oth[1], xx)
        packed = jnp.stack([a0, b0, a1, b1])
        g_eps = len(RELS) * per_eps
        packed = packed.reshape(g_eps, span + 1, adim)
        x_g = packed[:, :span].reshape(g_eps * span, adim).astype(BF)
        temb = time_embed(packed[:, span, 0], expert)
        table = jnp.concatenate(
            [
                action_in.astype(F32),
                head_w.astype(F32).T,
                temb,
                attn_gain[None],
                mlp_gain[None],
                final_gain[None],
            ],
            axis=0,
        )
        table = blocks_of(table, expert_index, per_col)
        action_p = table[:adim].astype(BF)
        head_p = table[adim : 2 * adim].astype(BF)
        temb = table[2 * adim : 2 * adim + g_eps]
        attn_g, mlp_g, final_g = (table[2 * adim + g_eps + k] for k in range(3))
        h0 = (dot(x_g, action_p).reshape(g_eps, span, expert) + temb[:, None, :]).reshape(
            g_eps * span, expert
        )
        own_rows = per_eps * span
        h0_own = h0[:own_rows]
        an = rms(h0, attn_g).astype(BF)
        mid = expert // nc

        def group_rows(values):
            return [values[k * own_rows : (k + 1) * own_rows] for k in range(len(RELS))]

        qa_out = dot(an[:, :mid], qa_own) + dot(an[:, mid:], qa_oth)
        q_part = (qa_out[:, :heads_cols] * hd ** (-0.5)).astype(BF)
        qa_out = jnp.concatenate([q_part, qa_out[:, heads_cols:].astype(BF)], axis=1)
        qa_in = exchange(group_rows(qa_out))
        heads = len(RELS) * heads_cols // hd
        query = jnp.stack([q[:, :heads_cols] for q in qa_in], axis=0)
        query = query.reshape(len(RELS), own_rows, heads_cols // hd, hd).transpose(0, 2, 1, 3)
        query = query.reshape(heads, own_eps, span, hd).transpose(1, 0, 2, 3)
        query = query.reshape(own_eps, heads * span, hd)
        parts = [q[:, heads_cols:] for q in qa_in]
        same = jnp.concatenate(order(parts[0], parts[1], ii), axis=1)
        diff = jnp.concatenate(order(parts[2], parts[3], ii), axis=1)
        akeys, avals = (t.reshape(own_eps, span, hd) for t in order(same, diff, xx))

        pn = normed_blocks(
            prefix_hidden.reshape(own_eps * positions, width), prefix_gain, prefix_index, half
        )
        wide = width // nc
        proj_same = (dot(pn[:, :wide], kv_same) + dot(pn[:, wide:], kv_same_c)).astype(BF)
        proj_diff = (dot(pn[:, :wide], kv_diff) + dot(pn[:, wide:], kv_diff_c)).astype(BF)
        pkeys, pvals = (
            t.reshape(own_eps, positions, hd) for t in order(proj_same, proj_diff, xx)
        )

        lens = lax.dynamic_slice_in_dim(prefix_len, member * per_eps, per_eps, 0)
        live = jnp.arange(positions, dtype=jnp.int32)[None, :] < lens[:, None]
        scores = jnp.einsum("erd,epd->erp", query, pkeys, preferred_element_type=F32)
        probs = jnp.where(live[:, None, :], jnp.exp(scores), 0.0)
        a_scores = jnp.einsum("erd,ecd->erc", query, akeys, preferred_element_type=F32)
        a_probs = jnp.exp(a_scores)
        denom = jnp.sum(probs, axis=-1) + jnp.sum(a_probs, axis=-1)
        weighted = jnp.einsum("erp,epd->erd", probs.astype(BF), pvals, preferred_element_type=F32)
        weighted = weighted + jnp.einsum(
            "erc,ecd->erd", a_probs.astype(BF), avals, preferred_element_type=F32
        )
        attn = (weighted / denom[:, :, None]).astype(BF)

        attn = attn.reshape(own_eps, heads, span, hd).transpose(0, 2, 1, 3)
        attn = attn.reshape(own_rows, len(RELS), heads_cols)
        out_own = jnp.concatenate(ring(out_w), axis=1)
        out_all = spread(out_own)
        out_c = [flip(t, "c") for t in out_all]
        mine = sum(dot(attn[:, k], out_all[k]) for k in range(len(RELS)))
        theirs = sum(dot(attn[:, k], out_c[k]) for k in range(len(RELS)))
        h1 = h0_own + jnp.concatenate([mine, theirs], axis=1)

        gu_own = jnp.concatenate(ring(jnp.concatenate([gate_w, up_w], axis=1)), axis=0)
        gu_oth = flip(gu_own, "c")
        down_own = jnp.concatenate(ring(down_w), axis=1)
        down_oth = flip(down_own, "c")
        mn = rms(h1, mlp_g).astype(BF)
        mn = jnp.concatenate(spread(mn), axis=0)
        gu = dot(mn[:, :mid], gu_own) + dot(mn[:, mid:], gu_oth)
        units = gate_w.shape[1]
        hidden = (jax.nn.gelu(gu[:, :units], approximate=True) * gu[:, units:]).astype(BF)
        ff = jnp.concatenate([dot(hidden, down_own), dot(hidden, down_oth)], axis=1)
        ff_rows = group_rows(ff)
        ff_in = exchange([ff_rows[0]] + [t.astype(BF) for t in ff_rows[1:]])
        h2 = h1 + sum(t.astype(F32) for t in ff_in)

        final = rms(h2, final_g).astype(BF)
        velocity = lax.dot_general(
            final, head_p, (((1,), (1,)), ((), ())), preferred_element_type=F32
        ).reshape(own_eps, span, adim)
        target = noise - actions
        own_target = lax.dynamic_slice_in_dim(target, member * per_eps, per_eps, 0)
        diff = velocity - own_target
        return velocity, jnp.mean(diff * diff, axis=(1, 2))

    return on_device


def solution(mesh):
    ndp, nmp = mesh.shape["dp"], mesh.shape["mp"]
    sizes = (ndp // 2, 2, nmp // 2, 2)
    fine = Mesh(mesh.devices.reshape(sizes), ("o", "i", "x", "c"))
    dp, mp, every = ("o", "i"), ("x", "c"), ("o", "i", "x", "c")
    in_specs = (
        P(every, None, None),
        P(dp),
        P(dp, None, None),
        P(dp, None, None),
        P(dp),
        P(),
        P(dp, None),
        P(dp, None),
        P(),
        P(),
        P(dp, mp),
        P(dp, None),
        P(dp, None),
        P(mp, dp),
        P(),
        P(dp, mp),
        P(dp, mp),
        P(mp, dp),
        P(),
        P(),
    )
    out_specs = (P(every, None, None), P(every))
    return jax.shard_map(
        make(*sizes), mesh=fine, in_specs=in_specs, out_specs=out_specs, check_vma=False
    )
```

```python
import math

import jax
import jax.numpy as jnp
from jax import lax
from jax.experimental import pallas as pl
from jax.experimental.pallas import tpu as pltpu
from jax.sharding import Mesh
from jax.sharding import PartitionSpec as P


TSTEPS = 1000
BF = jnp.bfloat16
F32 = jnp.float32
LANES = 128
PAD = 64
DP, MP = ("o", "i"), ("x", "c")
RELS = ((0, 0), (1, 0), (0, 1), (1, 1))


def rms(values, gain):
    return values * lax.rsqrt(jnp.mean(values * values, axis=-1, keepdims=True) + 1e-06) * gain


def time_embed(times, width):
    half = width // 2
    steps = jnp.arange(half, dtype=jnp.float32)
    period = 0.004 * jnp.power(jnp.float32(1000.0), steps / (half - 1))
    angle = times[:, None] * (2.0 * math.pi) / period[None, :]
    return jnp.concatenate([jnp.sin(angle), jnp.cos(angle)], axis=-1)


def attend(query, pkeys, pvals, akeys, avals, lengths):
    live = jnp.arange(pkeys.shape[1], dtype=jnp.int32)[None, :] < lengths[:, None]
    scores = jnp.einsum("erd,epd->erp", query, pkeys, preferred_element_type=jnp.float32)
    probs = jnp.where(live[:, None, :], jnp.exp(scores), 0.0)
    action_scores = jnp.einsum("erd,ecd->erc", query, akeys, preferred_element_type=jnp.float32)
    action_probs = jnp.exp(action_scores)
    denom = jnp.sum(probs, axis=-1) + jnp.sum(action_probs, axis=-1)
    weighted = jnp.einsum(
        "erp,epd->erd", probs.astype(jnp.bfloat16), pvals, preferred_element_type=jnp.float32
    )
    weighted = weighted + jnp.einsum(
        "erc,ecd->erd", action_probs.astype(jnp.bfloat16), avals, preferred_element_type=jnp.float32
    )
    return (weighted / denom[:, :, None]).astype(jnp.bfloat16)


def gather_all(
    prefix_hidden,
    prefix_len,
    actions,
    noise,
    time_index,
    prefix_gain,
    key_weight,
    value_weight,
    action_in,
    attn_gain,
    query_w,
    akey_w,
    avalue_w,
    out_w,
    mlp_gain,
    gate_w,
    up_w,
    down_w,
    final_gain,
    head_w,
):
    own_eps, positions, width = prefix_hidden.shape
    group_eps, span, adim = actions.shape
    expert = action_in.shape[1]
    head_size = key_weight.shape[1]
    local_heads = query_w.shape[1] // head_size
    rows_total = group_eps * span
    own_rows = own_eps * span
    member = lax.axis_index(MP)
    first_row = member * own_rows
    first_ep = member * own_eps
    times = (time_index.astype(jnp.float32) + 0.5) / TSTEPS
    x_t = times[:, None, None] * noise + (1.0 - times)[:, None, None] * actions
    target = noise - actions
    x_in = x_t.reshape(rows_total, adim).astype(jnp.bfloat16)
    temb = time_embed(times, expert)
    h0 = (
        jnp.dot(x_in, action_in, preferred_element_type=jnp.float32).reshape(
            group_eps, span, expert
        )
        + temb[:, None, :]
    )
    h0 = h0.reshape(rows_total, expert)
    key_full, value_full = (
        lax.all_gather(key_weight, DP, axis=0, tiled=True),
        lax.all_gather(value_weight, DP, axis=0, tiled=True),
    )
    prefix_normed = rms(
        prefix_hidden.reshape(own_eps * positions, width).astype(jnp.float32), prefix_gain
    ).astype(jnp.bfloat16)
    pkeys = (
        jnp.dot(prefix_normed, key_full, preferred_element_type=jnp.float32)
        .astype(jnp.bfloat16)
        .reshape(own_eps, positions, head_size)
    )
    pvals = (
        jnp.dot(prefix_normed, value_full, preferred_element_type=jnp.float32)
        .astype(jnp.bfloat16)
        .reshape(own_eps, positions, head_size)
    )
    normed = rms(h0, attn_gain).astype(jnp.bfloat16)
    query_full, akey_full, avalue_full = (
        lax.all_gather(query_w, DP, axis=0, tiled=True),
        lax.all_gather(akey_w, DP, axis=0, tiled=True),
        lax.all_gather(avalue_w, DP, axis=0, tiled=True),
    )
    query = (
        jnp.dot(normed, query_full, preferred_element_type=jnp.float32) * head_size ** (-0.5)
    ).astype(jnp.bfloat16)
    akeys = (
        jnp.dot(normed, akey_full, preferred_element_type=jnp.float32)
        .astype(jnp.bfloat16)
        .reshape(group_eps, span, head_size)
    )
    avals = (
        jnp.dot(normed, avalue_full, preferred_element_type=jnp.float32)
        .astype(jnp.bfloat16)
        .reshape(group_eps, span, head_size)
    )
    keys_all, vals_all = (
        lax.all_gather(pkeys, MP, axis=0, tiled=True),
        lax.all_gather(pvals, MP, axis=0, tiled=True),
    )
    attn = attend(
        query.reshape(group_eps, span * local_heads, head_size),
        keys_all,
        vals_all,
        akeys,
        avals,
        prefix_len,
    )
    attn = attn.reshape(rows_total, local_heads * head_size)
    out_full = lax.all_gather(out_w, DP, axis=1, tiled=True)
    gate_full, up_full = (
        lax.all_gather(gate_w, DP, axis=0, tiled=True),
        lax.all_gather(up_w, DP, axis=0, tiled=True),
    )
    down_full = lax.all_gather(down_w, DP, axis=1, tiled=True)
    h0_own = lax.dynamic_slice_in_dim(h0, first_row, own_rows, 0)
    h1 = h0_own + lax.psum_scatter(
        jnp.dot(attn, out_full, preferred_element_type=jnp.float32).astype(jnp.bfloat16),
        MP,
        scatter_dimension=0,
        tiled=True,
    ).astype(jnp.float32)
    mixed_own = rms(h1, mlp_gain).astype(jnp.bfloat16)
    mixed = lax.all_gather(mixed_own, MP, axis=0, tiled=True)
    gate = jnp.dot(mixed, gate_full, preferred_element_type=jnp.float32)
    upper = jnp.dot(mixed, up_full, preferred_element_type=jnp.float32)
    hidden = (jax.nn.gelu(gate, approximate=True) * upper).astype(jnp.bfloat16)
    h2 = h1 + lax.psum_scatter(
        jnp.dot(hidden, down_full, preferred_element_type=jnp.float32).astype(jnp.bfloat16),
        MP,
        scatter_dimension=0,
        tiled=True,
    ).astype(jnp.float32)
    final = rms(h2, final_gain).astype(jnp.bfloat16)
    velocity = jnp.dot(final, head_w, preferred_element_type=jnp.float32).reshape(
        own_eps, span, adim
    )
    own_target = lax.dynamic_slice_in_dim(target, first_ep, own_eps, 0)
    diff = velocity - own_target
    ep_loss = jnp.mean(diff * diff, axis=(1, 2))
    return (velocity, ep_loss)


def dot(a, b):
    return jnp.dot(a, b, preferred_element_type=F32)


def after(values, *earlier):
    return lax.optimization_barrier((values,) + earlier)[0]


def at(*block):
    return pl.BlockSpec(block, lambda *s: (0,) * len(block))


def like(*shape, dtype=BF):
    return jax.ShapeDtypeStruct(shape, dtype)


def split_rows(total, rows, outs):
    outs[0][...] = total[:rows].astype(outs[0].dtype)
    for k in range(1, len(outs)):
        outs[k][...] = total[PAD * k : PAD * k + rows].astype(outs[k].dtype)


def pack_weights(query_w, akey_w, avalue_w, key_w, value_w, down_w, out_w, gate_w, up_w):
    rows, hq = query_w.shape
    ha, hk = akey_w.shape[1], key_w.shape[1]
    quarter, half = ha // 2, key_w.shape[0] // 2
    nd, units = down_w.shape[0], gate_w.shape[1]

    def kernel(q, ak, av, kw, vw, dw, ow, gw, uw, first, od, gu):
        xx, cc = lax.axis_index("x"), lax.axis_index("c")
        cols = pl.ds(pl.multiple_of(cc * quarter, quarter), quarter)
        part = pl.ds(pl.multiple_of(cc * half, half), half)
        first[:, :hq] = q[...]

        @pl.when(xx == 0)
        def _():
            first[:, hq : hq + quarter] = ak[:, cols]
            first[:, hq + quarter :] = kw[part, :]

        @pl.when(xx != 0)
        def _():
            first[:, hq : hq + quarter] = av[:, cols]
            first[:, hq + quarter :] = vw[part, :]

        od[:nd] = dw[...]
        od[nd:] = ow[...]
        gu[:, :units] = gw[...]
        gu[:, units:] = uw[...]

    return pl.pallas_call(
        kernel,
        out_shape=(
            like(rows, hq + quarter + hk),
            like(nd + out_w.shape[0], down_w.shape[1]),
            like(rows, 2 * units),
        ),
        name="pack_weights",
    )(query_w, akey_w, avalue_w, key_w, value_w, down_w, out_w, gate_w, up_w)


def expert_in(x_g, temb, action_in, attn_gain, mlp_gain, final_gain, head_w, span, per):
    rows = x_g.shape[0]
    groups, width = temb.shape
    adim = head_w.shape[0]
    count = width // per

    def kernel(x, te, act, ga, gm, gf, hw, an, h0, gains, head_p, h_all):
        oo, cc = lax.axis_index("o"), lax.axis_index("c")
        for b in range(count):
            r, c = b % (count // 2), b // (count // 2)
            block = (oo ^ r) * 2 + (cc ^ c)
            src = pl.ds(pl.multiple_of(block * per, per), per)
            dst = slice(b * per, (b + 1) * per)
            h = dot(x[...], act[:, src])
            for k in range(groups):
                h_all[PAD * k : PAD * (k + 1), dst] = h[PAD * k : PAD * (k + 1)] + te[k : k + 1, src]
            gains[0:1, dst] = gm[:, src]
            gains[1:2, dst] = gf[:, src]
            gains[2:3, dst] = ga[:, src]
            head_p[:, dst] = hw[:, src]
        h = h_all[...]
        h0[...] = h[:span]
        an[...] = (
            h * lax.rsqrt(jnp.mean(h * h, axis=-1, keepdims=True) + 1e-06) * gains[2:3, :]
        ).astype(BF)

    return pl.pallas_call(
        kernel,
        out_shape=(
            like(rows, width),
            like(span, width, dtype=F32),
            like(8, width, dtype=F32),
            like(adim, width),
        ),
        scratch_shapes=[pltpu.VMEM((rows, width), F32)],
        name="expert_in",
    )(
        x_g,
        temb,
        action_in,
        attn_gain.reshape(1, width),
        mlp_gain.reshape(1, width),
        final_gain.reshape(1, width),
        head_w,
    )


def unpack_first(got, cols):
    rows, total = got[0].shape
    count = len(got)

    def kernel(*refs):
        qa, kv = refs[count:]
        for r in range(count):
            qa[r * rows : (r + 1) * rows] = refs[r][:, :cols]
            kv[r * rows : (r + 1) * rows] = refs[r][:, cols:]

    return pl.pallas_call(
        kernel,
        out_shape=(like(count * rows, cols), like(count * rows, total - cols)),
        name="unpack_first",
    )(*got)


def queries(an, own, other, heads_cols, scale, span):
    mid, cols = own.shape

    def kernel(a, w0, w1, *refs):
        outs, total = refs[:-1], refs[-1]
        v = dot(a[:, :mid], w0[...]) + dot(a[:, mid:], w1[...])
        total[:, :heads_cols] = v[:, :heads_cols] * scale
        total[:, heads_cols:] = v[:, heads_cols:]
        split_rows(total[...], span, outs)

    return pl.pallas_call(
        kernel,
        out_shape=[like(span, cols) for _ in RELS],
        scratch_shapes=[pltpu.VMEM((an.shape[0], cols), F32)],
        name="queries",
    )(an, own, other)


def attention(prefix, gain, kv_own, kv_oth, qa, length, heads_cols):
    positions, width = prefix.shape
    tall, hd = kv_own[0].shape
    span, qa_cols = qa[0].shape
    per_part = heads_cols // hd
    heads = len(RELS) * per_part
    step = 512
    steps = positions // step
    count = 16
    per = width // count
    no = count // 4

    def kernel(len_ref, x, g, *refs):
        own, oth, qs = refs[0:4], refs[4:8], refs[8:12]
        outs = refs[12:16]
        q_all, pn, acc, den = refs[16:20]
        s = pl.program_id(0)
        oo, ii, xx, cc = (lax.axis_index(n) for n in ("o", "i", "x", "c"))

        @pl.when(s == 0)
        def _():
            q_all[...] = jnp.zeros_like(q_all)
            for k in range(len(RELS)):
                for h in range(per_part):
                    q_all[PAD * (k * per_part + h) : PAD * (k * per_part + h) + span] = qs[k][
                        :, h * hd : (h + 1) * hd
                    ]
            acc[...] = jnp.zeros_like(acc)
            den[...] = jnp.zeros_like(den)

        v = x[...].astype(F32)
        scale = lax.rsqrt(jnp.mean(v * v, axis=-1, keepdims=True) + 1e-06)
        for b in range(count):
            r, i, c = b % no, (b // no) % 2, b // (2 * no)
            block = ((oo ^ r) * 2 + (cc ^ c)) * 2 + (ii ^ i)
            src = pl.ds(pl.multiple_of(block * per, per), per)
            pn[:, b * per : (b + 1) * per] = (x[:, src].astype(F32) * scale * g[:, src]).astype(BF)
        same = diff = 0.0
        for c, refs_c in enumerate((own, oth)):
            for i in range(2):
                m = pn[:, (c * 2 + i) * tall : (c * 2 + i + 1) * tall]
                same = same + dot(m, refs_c[i][...])
                diff = diff + dot(m, refs_c[2 + i][...])
        first = xx == 0
        same, diff = same.astype(BF), diff.astype(BF)
        keys = jnp.where(first, same, diff)
        vals = jnp.where(first, diff, same)
        nt = (((1,), (1,)), ((), ()))
        sc = lax.dot_general(q_all[...], keys, nt, preferred_element_type=F32)
        spot = s * step + lax.broadcasted_iota(jnp.int32, sc.shape, 1)
        p = jnp.where(spot < len_ref[0], jnp.exp(sc), 0.0)
        den[...] += jnp.sum(p, axis=-1, keepdims=True)
        acc[...] += dot(p.astype(BF), vals)

        @pl.when(s == steps - 1)
        def _():
            parts = [q[:, heads_cols:] for q in qs]
            flat = ii == 0
            lo = [jnp.where(flat, parts[2 * k], parts[2 * k + 1]) for k in range(2)]
            hi = [jnp.where(flat, parts[2 * k + 1], parts[2 * k]) for k in range(2)]
            sa = jnp.concatenate([lo[0], hi[0]], axis=1)
            da = jnp.concatenate([lo[1], hi[1]], axis=1)
            ak, av = jnp.where(first, sa, da), jnp.where(first, da, sa)
            pa = jnp.exp(lax.dot_general(q_all[...], ak, nt, preferred_element_type=F32))
            total = den[...] + jnp.sum(pa, axis=-1, keepdims=True)
            res = ((acc[...] + dot(pa.astype(BF), av)) / total).astype(BF)
            for k in range(len(RELS)):
                for h in range(per_part):
                    n = PAD * (k * per_part + h)
                    outs[k][:, h * hd : (h + 1) * hd] = res[n : n + span]

    return pl.pallas_call(
        kernel,
        grid=(steps,),
        out_shape=[like(span, heads_cols) for _ in RELS],
        in_specs=[
            pl.BlockSpec(memory_space=pltpu.SMEM),
            pl.BlockSpec((step, width), lambda s: (s, 0)),
            at(1, width),
        ]
        + [at(tall, hd)] * 8
        + [at(span, qa_cols)] * 4,
        out_specs=[at(span, heads_cols)] * 4,
        scratch_shapes=[
            pltpu.VMEM((PAD * heads, hd), BF),
            pltpu.VMEM((step, width), BF),
            pltpu.VMEM((PAD * heads, hd), F32),
            pltpu.VMEM((PAD * heads, 1), F32),
        ],
        name="prefix_attention",
    )(length, prefix, gain.reshape(1, width), *kv_own, *kv_oth, *qa)


def row_outs(rows, width, parts):
    return [like(rows, width, dtype=F32)] + [like(rows, width) for _ in range(parts - 1)]


def out_project(attn, pieces, units):
    rows = attn[0].shape[0]
    parts, count = len(attn), len(pieces)
    tall, cols = pieces[0].shape
    place = tall // units - 1

    def kernel(*refs):
        a_refs, w_refs = refs[:parts], refs[parts : parts + count]
        outs, a_all, total = refs[parts + count : -2], refs[-2], refs[-1]
        for k in range(parts):
            a_all[PAD * k : PAD * k + rows] = a_refs[k][...]
        for b in range(0, count, 2):
            pair = jnp.concatenate([w_refs[b][...], w_refs[b + 1][...]], axis=1)
            total[:, b * cols : (b + 2) * cols] = dot(a_all[...], pair)
        split_rows(total, rows, outs)

    return pl.pallas_call(
        kernel,
        grid=(1,),
        out_shape=row_outs(rows, count * cols, parts),
        in_specs=[at(rows, units)] * parts
        + [pl.BlockSpec((units, cols), lambda s: (place, 0))] * count,
        out_specs=[at(rows, count * cols)] * parts,
        scratch_shapes=[
            pltpu.VMEM((PAD * parts, units), BF),
            pltpu.VMEM((PAD * parts, count * cols), F32),
        ],
        name="out_project",
    )(*attn, *pieces)


def feed_forward(mn, gu, od, units):
    rows = mn[0].shape[0]
    parts, count = len(mn), len(gu)
    per, cols = gu[0].shape[0], od[0].shape[1]
    step = 256
    steps = units // step

    def kernel(*refs):
        m_refs, refs = refs[:parts], refs[parts:]
        g_refs, u_refs, d_refs = refs[:count], refs[count : 2 * count], refs[2 * count : 3 * count]
        outs, m_all, total = refs[3 * count : -2], refs[-2], refs[-1]
        s = pl.program_id(0)

        @pl.when(s == 0)
        def _():
            for k in range(parts):
                m_all[PAD * k : PAD * k + rows] = m_refs[k][...]
            total[...] = jnp.zeros_like(total)

        gate = dot(m_all[...], jnp.concatenate([g[...] for g in g_refs], axis=0))
        up = dot(m_all[...], jnp.concatenate([u[...] for u in u_refs], axis=0))
        hid = (jax.nn.gelu(gate, approximate=True) * up).astype(BF)
        for b in range(0, count, 2):
            pair = jnp.concatenate([d_refs[b][...], d_refs[b + 1][...]], axis=1)
            total[:, b * cols : (b + 2) * cols] += dot(hid, pair)

        @pl.when(s == steps - 1)
        def _():
            split_rows(total, rows, outs)

    return pl.pallas_call(
        kernel,
        grid=(steps,),
        out_shape=row_outs(rows, count * cols, parts),
        in_specs=[at(rows, count * per)] * parts
        + [pl.BlockSpec((per, step), lambda s: (0, s))] * count
        + [pl.BlockSpec((per, step), lambda s: (0, s + steps))] * count
        + [pl.BlockSpec((step, cols), lambda s: (s, 0))] * count,
        out_specs=[at(rows, count * cols)] * parts,
        scratch_shapes=[
            pltpu.VMEM((PAD * parts, count * per), BF),
            pltpu.VMEM((PAD * parts, count * cols), F32),
        ],
        name="feed_forward",
    )(*mn, *gu, *gu, *od)


def make(no, ni, nx, nc):
    def flip(value, axis):
        return lax.ppermute(value, axis, [(0, 1), (1, 0)])

    def cross(value, di, dx):
        pairs = [
            (i * nx + x, (i ^ di) * nx + (x ^ dx)) for i in range(ni) for x in range(nx)
        ]
        return lax.ppermute(value, ("i", "x"), pairs)

    def spread(value):
        return [value] + [cross(value, di, dx) for di, dx in RELS[1:]]

    def exchange(parts):
        return [parts[0]] + [cross(p, di, dx) for p, (di, dx) in zip(parts[1:], RELS[1:])]

    def turned(value, r):
        return lax.ppermute(
            value,
            ("o", "i", "c"),
            [
                ((o * ni + i) * nc + c, ((o ^ r) * ni + c) * nc + i)
                for o in range(no)
                for i in range(ni)
                for c in range(nc)
            ],
        )

    def hop(value, pairs):
        return lax.ppermute(value, "o", pairs)

    def partner(r):
        return [(o, o ^ r) for o in range(no)]

    MIDDLE, OUTWARD = [(1, 2), (2, 1)], [(1, 0), (2, 3)]

    def fast(
        prefix_hidden,
        prefix_len,
        actions,
        noise,
        time_index,
        prefix_gain,
        key_weight,
        value_weight,
        action_in,
        attn_gain,
        query_w,
        akey_w,
        avalue_w,
        out_w,
        mlp_gain,
        gate_w,
        up_w,
        down_w,
        final_gain,
        head_w,
):
        own_eps, positions, width = prefix_hidden.shape
        _, span, adim = actions.shape
        expert = action_in.shape[1]
        hd = key_weight.shape[1]
        heads_cols = query_w.shape[1]
        units = gate_w.shape[1]
        oo, xx, cc = (lax.axis_index(a) for a in ("o", "x", "c"))
        member = xx * nc + cc

        def order(first, second, at_one):
            return jnp.where(at_one == 0, first, second), jnp.where(at_one == 0, second, first)

        first, od, gu = pack_weights(
            query_w, akey_w, avalue_w, key_weight, value_weight, down_w, out_w, gate_w, up_w
        )
        got = [turned(first, r) for r in range(no)]
        od_0, gu_0 = turned(od, 0), turned(gu, 0)

        times = (time_index.astype(F32) + 0.5) / TSTEPS
        x_t = times[:, None, None] * noise + (1.0 - times)[:, None, None] * actions
        x_in = x_t.astype(BF)

        def mine_of(values):
            v = values.reshape((nx, nc) + values.shape[1:])
            return lax.dynamic_index_in_dim(v, cc, 1, keepdims=False)

        packed = jnp.concatenate(
            [
                mine_of(x_in).astype(F32),
                jnp.broadcast_to(mine_of(times)[:, None, None], (nx, 1, adim)),
            ],
            axis=1,
        )
        packed_oth = flip(packed, "i")
        a0, a1 = order(packed[0], packed[1], xx)
        b0, b1 = order(packed_oth[0], packed_oth[1], xx)
        packed = jnp.stack([a0, b0, a1, b1])
        temb = time_embed(packed[:, span, 0], expert)
        x_g = jnp.pad(packed[:, :span], ((0, 0), (0, PAD - span), (0, 0))).astype(BF)
        an, h0, gains, head_p = expert_in(
            x_g.reshape(len(RELS) * PAD, adim),
            temb,
            action_in,
            attn_gain,
            mlp_gain,
            final_gain,
            head_w.T,
            span,
            expert // (no * nc),
        )

        got = [after(t, an) for t in got]
        qa_own, kv = unpack_first(got, first.shape[1] - hd)
        kv_all = spread(kv)
        od_got = [od_0] + [hop(after(od_0, qa_own), partner(r)) for r in range(1, no)]
        qa_oth = flip(qa_own, "c")
        q_parts = queries(an, qa_own, qa_oth, heads_cols, hd ** (-0.5), span)
        qa = exchange(q_parts)
        gu_t = after(gu_0, q_parts[0])
        gu_a, gu_b = hop(gu_t, partner(1)), hop(gu_t, MIDDLE)
        kv_all = [after(t, q_parts[0]) for t in kv_all]
        kv_oth = [flip(t, "c") for t in kv_all]
        length = lax.dynamic_slice_in_dim(prefix_len, member, 1, 0)
        attn = attention(
            prefix_hidden.reshape(positions, width),
            prefix_gain,
            kv_all,
            kv_oth,
            qa,
            length,
            heads_cols,
        )

        attn_in = exchange(attn)
        gu_c, gu_d = hop(after(gu_b, attn[0]), OUTWARD), hop(after(gu_a, attn[0]), MIDDLE)
        od_all = od_got + [flip(after(t, attn[0]), "c") for t in od_got]
        out_parts = out_project(attn_in, od_all, heads_cols)
        out_in = exchange(out_parts)
        gu_e = hop(after(gu_d, out_parts[0]), OUTWARD)
        h1 = h0 + sum(t.astype(F32) for t in out_in)

        mn = spread(rms(h1, gains[0]).astype(BF))
        inner = (oo == 1) | (oo == 2)
        gu_t, gu_a, gu_b, gu_c, gu_d, gu_e = (
            after(t, h1) for t in (gu_t, gu_a, gu_b, gu_c, gu_d, after(gu_e, *mn))
        )
        gu_got = [gu_t, gu_a, jnp.where(inner, gu_d, gu_c), jnp.where(inner, gu_b, gu_e)]
        gu_all = gu_got + [flip(t, "c") for t in gu_got]
        ff_parts = feed_forward(mn, gu_all, od_all, units)
        h2 = h1 + sum(t.astype(F32) for t in exchange(ff_parts))

        final = rms(h2, gains[1]).astype(BF)
        velocity = lax.dot_general(
            final, head_p, (((1,), (1,)), ((), ())), preferred_element_type=F32
        )
        target = noise - actions
        own_target = lax.dynamic_slice_in_dim(target, member, own_eps, 0)
        velocity = velocity.reshape(own_eps, span, adim)
        diff = velocity - own_target
        return velocity, jnp.mean(diff * diff, axis=(1, 2))

    def on_device(*values):
        eps, positions, _ = values[0].shape
        expert = values[8].shape[1]
        fits = (
            (no, ni, nx, nc) == (4, 2, 2, 2)
            and eps == 1
            and values[2].shape[1] <= PAD
            and positions % 256 == 0
            and (expert // (no * nc)) % LANES == 0
            and values[6].shape[0] == 2 * values[10].shape[0] == 2 * values[13].shape[1]
        )
        if not fits:
            return gather_all(*values)
        return fast(*values)

    return on_device


def solution(mesh):
    in_specs = (
        P(("dp", "mp"), None, None),
        P("dp"),
        P("dp", None, None),
        P("dp", None, None),
        P("dp"),
        P(),
        P("dp", None),
        P("dp", None),
        P(),
        P(),
        P("dp", "mp"),
        P("dp", None),
        P("dp", None),
        P("mp", "dp"),
        P(),
        P("dp", "mp"),
        P("dp", "mp"),
        P("mp", "dp"),
        P(),
        P(),
    )
    out_specs = (P(("dp", "mp"), None, None), P(("dp", "mp")))
    ndp, nmp = mesh.shape["dp"], mesh.shape["mp"]
    sizes = (ndp // 2, 2, nmp // 2, 2)
    fine = Mesh(mesh.devices.reshape(sizes), DP + MP)
    names = {"dp": DP, "mp": MP}

    def finer(spec):
        flat = []
        for entry in spec:
            entry = (entry,) if isinstance(entry, str) else entry
            flat.append(None if entry is None else tuple(n for e in entry for n in names[e]))
        return P(*flat)

    return jax.shard_map(
        make(*sizes),
        mesh=fine,
        in_specs=tuple(finer(s) for s in in_specs),
        out_specs=tuple(finer(s) for s in out_specs),
        check_vma=False,
    )
```

```python
import math

import jax
import jax.numpy as jnp
from jax import lax
from jax.experimental import pallas as pl
from jax.experimental.pallas import tpu as pltpu
from jax.sharding import Mesh
from jax.sharding import PartitionSpec as P


TSTEPS = 1000
BF = jnp.bfloat16
F32 = jnp.float32
LANES = 128
PAD = 64
DP, MP = ("o", "i"), ("x", "c")
RELS = ((0, 0), (1, 0), (0, 1), (1, 1))


def rms(values, gain):
    return values * lax.rsqrt(jnp.mean(values * values, axis=-1, keepdims=True) + 1e-06) * gain


def time_embed(times, width):
    half = width // 2
    steps = jnp.arange(half, dtype=jnp.float32)
    period = 0.004 * jnp.power(jnp.float32(1000.0), steps / (half - 1))
    angle = times[:, None] * (2.0 * math.pi) / period[None, :]
    return jnp.concatenate([jnp.sin(angle), jnp.cos(angle)], axis=-1)


def attend(query, pkeys, pvals, akeys, avals, lengths):
    live = jnp.arange(pkeys.shape[1], dtype=jnp.int32)[None, :] < lengths[:, None]
    scores = jnp.einsum("erd,epd->erp", query, pkeys, preferred_element_type=jnp.float32)
    probs = jnp.where(live[:, None, :], jnp.exp(scores), 0.0)
    action_scores = jnp.einsum("erd,ecd->erc", query, akeys, preferred_element_type=jnp.float32)
    action_probs = jnp.exp(action_scores)
    denom = jnp.sum(probs, axis=-1) + jnp.sum(action_probs, axis=-1)
    weighted = jnp.einsum(
        "erp,epd->erd", probs.astype(jnp.bfloat16), pvals, preferred_element_type=jnp.float32
    )
    weighted = weighted + jnp.einsum(
        "erc,ecd->erd", action_probs.astype(jnp.bfloat16), avals, preferred_element_type=jnp.float32
    )
    return (weighted / denom[:, :, None]).astype(jnp.bfloat16)


def gather_all(
    prefix_hidden,
    prefix_len,
    actions,
    noise,
    time_index,
    prefix_gain,
    key_weight,
    value_weight,
    action_in,
    attn_gain,
    query_w,
    akey_w,
    avalue_w,
    out_w,
    mlp_gain,
    gate_w,
    up_w,
    down_w,
    final_gain,
    head_w,
):
    own_eps, positions, width = prefix_hidden.shape
    group_eps, span, adim = actions.shape
    expert = action_in.shape[1]
    head_size = key_weight.shape[1]
    local_heads = query_w.shape[1] // head_size
    rows_total = group_eps * span
    own_rows = own_eps * span
    member = lax.axis_index(MP)
    first_row = member * own_rows
    first_ep = member * own_eps
    times = (time_index.astype(jnp.float32) + 0.5) / TSTEPS
    x_t = times[:, None, None] * noise + (1.0 - times)[:, None, None] * actions
    target = noise - actions
    x_in = x_t.reshape(rows_total, adim).astype(jnp.bfloat16)
    temb = time_embed(times, expert)
    h0 = (
        jnp.dot(x_in, action_in, preferred_element_type=jnp.float32).reshape(
            group_eps, span, expert
        )
        + temb[:, None, :]
    )
    h0 = h0.reshape(rows_total, expert)
    key_full, value_full = (
        lax.all_gather(key_weight, DP, axis=0, tiled=True),
        lax.all_gather(value_weight, DP, axis=0, tiled=True),
    )
    prefix_normed = rms(
        prefix_hidden.reshape(own_eps * positions, width).astype(jnp.float32), prefix_gain
    ).astype(jnp.bfloat16)
    pkeys = (
        jnp.dot(prefix_normed, key_full, preferred_element_type=jnp.float32)
        .astype(jnp.bfloat16)
        .reshape(own_eps, positions, head_size)
    )
    pvals = (
        jnp.dot(prefix_normed, value_full, preferred_element_type=jnp.float32)
        .astype(jnp.bfloat16)
        .reshape(own_eps, positions, head_size)
    )
    normed = rms(h0, attn_gain).astype(jnp.bfloat16)
    query_full, akey_full, avalue_full = (
        lax.all_gather(query_w, DP, axis=0, tiled=True),
        lax.all_gather(akey_w, DP, axis=0, tiled=True),
        lax.all_gather(avalue_w, DP, axis=0, tiled=True),
    )
    query = (
        jnp.dot(normed, query_full, preferred_element_type=jnp.float32) * head_size ** (-0.5)
    ).astype(jnp.bfloat16)
    akeys = (
        jnp.dot(normed, akey_full, preferred_element_type=jnp.float32)
        .astype(jnp.bfloat16)
        .reshape(group_eps, span, head_size)
    )
    avals = (
        jnp.dot(normed, avalue_full, preferred_element_type=jnp.float32)
        .astype(jnp.bfloat16)
        .reshape(group_eps, span, head_size)
    )
    keys_all, vals_all = (
        lax.all_gather(pkeys, MP, axis=0, tiled=True),
        lax.all_gather(pvals, MP, axis=0, tiled=True),
    )
    attn = attend(
        query.reshape(group_eps, span * local_heads, head_size),
        keys_all,
        vals_all,
        akeys,
        avals,
        prefix_len,
    )
    attn = attn.reshape(rows_total, local_heads * head_size)
    out_full = lax.all_gather(out_w, DP, axis=1, tiled=True)
    gate_full, up_full = (
        lax.all_gather(gate_w, DP, axis=0, tiled=True),
        lax.all_gather(up_w, DP, axis=0, tiled=True),
    )
    down_full = lax.all_gather(down_w, DP, axis=1, tiled=True)
    h0_own = lax.dynamic_slice_in_dim(h0, first_row, own_rows, 0)
    h1 = h0_own + lax.psum_scatter(
        jnp.dot(attn, out_full, preferred_element_type=jnp.float32).astype(jnp.bfloat16),
        MP,
        scatter_dimension=0,
        tiled=True,
    ).astype(jnp.float32)
    mixed_own = rms(h1, mlp_gain).astype(jnp.bfloat16)
    mixed = lax.all_gather(mixed_own, MP, axis=0, tiled=True)
    gate = jnp.dot(mixed, gate_full, preferred_element_type=jnp.float32)
    upper = jnp.dot(mixed, up_full, preferred_element_type=jnp.float32)
    hidden = (jax.nn.gelu(gate, approximate=True) * upper).astype(jnp.bfloat16)
    h2 = h1 + lax.psum_scatter(
        jnp.dot(hidden, down_full, preferred_element_type=jnp.float32).astype(jnp.bfloat16),
        MP,
        scatter_dimension=0,
        tiled=True,
    ).astype(jnp.float32)
    final = rms(h2, final_gain).astype(jnp.bfloat16)
    velocity = jnp.dot(final, head_w, preferred_element_type=jnp.float32).reshape(
        own_eps, span, adim
    )
    own_target = lax.dynamic_slice_in_dim(target, first_ep, own_eps, 0)
    diff = velocity - own_target
    ep_loss = jnp.mean(diff * diff, axis=(1, 2))
    return (velocity, ep_loss)


def dot(a, b):
    return jnp.dot(a, b, preferred_element_type=F32)


def after(values, *earlier):
    return lax.optimization_barrier((values,) + earlier)[0]


def at(*block):
    return pl.BlockSpec(block, lambda *s: (0,) * len(block))


def grant(mib):
    return pltpu.CompilerParams(vmem_limit_bytes=mib * 2**20)


def like(*shape, dtype=BF):
    return jax.ShapeDtypeStruct(shape, dtype)


def split_rows(total, rows, outs):
    outs[0][...] = total[:rows].astype(outs[0].dtype)
    for k in range(1, len(outs)):
        outs[k][...] = total[PAD * k : PAD * k + rows].astype(outs[k].dtype)


def pack_weights(query_w, akey_w, avalue_w, key_w, value_w, gate_w, up_w):
    rows, hq = query_w.shape
    ha, hk = akey_w.shape[1], key_w.shape[1]
    quarter, half = ha // 2, key_w.shape[0] // 2
    units = gate_w.shape[1]

    def kernel(q, ak, av, kw, vw, gw, uw, first, gu):
        xx, cc = lax.axis_index("x"), lax.axis_index("c")
        cols = pl.ds(pl.multiple_of(cc * quarter, quarter), quarter)
        part = pl.ds(pl.multiple_of(cc * half, half), half)
        first[:, :hq] = q[...]

        @pl.when(xx == 0)
        def _():
            first[:, hq : hq + quarter] = ak[:, cols]
            first[:, hq + quarter :] = kw[part, :]

        @pl.when(xx != 0)
        def _():
            first[:, hq : hq + quarter] = av[:, cols]
            first[:, hq + quarter :] = vw[part, :]

        gu[:, :units] = gw[...]
        gu[:, units:] = uw[...]

    return pl.pallas_call(
        kernel,
        out_shape=(
            like(rows, hq + quarter + hk),
            like(rows, 2 * units),
        ),
        name="pack_weights",
    )(query_w, akey_w, avalue_w, key_w, value_w, gate_w, up_w)


def expert_in(x_g, temb, action_in, attn_gain, mlp_gain, final_gain, head_w, span, per):
    rows = x_g.shape[0]
    groups, width = temb.shape
    adim = head_w.shape[0]
    count = width // per

    def kernel(x, te, act, ga, gm, gf, hw, an, h0, gains, head_p, h_all):
        oo, cc = lax.axis_index("o"), lax.axis_index("c")
        for b in range(count):
            r, c = b % (count // 2), b // (count // 2)
            block = (oo ^ r) * 2 + (cc ^ c)
            src = pl.ds(pl.multiple_of(block * per, per), per)
            dst = slice(b * per, (b + 1) * per)
            h = dot(x[...], act[:, src])
            for k in range(groups):
                h_all[PAD * k : PAD * (k + 1), dst] = h[PAD * k : PAD * (k + 1)] + te[k : k + 1, src]
            gains[0:1, dst] = gm[:, src]
            gains[1:2, dst] = gf[:, src]
            gains[2:3, dst] = ga[:, src]
            head_p[:, dst] = hw[:, src]
        h = h_all[...]
        h0[...] = h[:span]
        an[...] = (
            h * lax.rsqrt(jnp.mean(h * h, axis=-1, keepdims=True) + 1e-06) * gains[2:3, :]
        ).astype(BF)

    return pl.pallas_call(
        kernel,
        out_shape=(
            like(rows, width),
            like(span, width, dtype=F32),
            like(8, width, dtype=F32),
            like(adim, width),
        ),
        scratch_shapes=[pltpu.VMEM((rows, width), F32)],
        name="expert_in",
    )(
        x_g,
        temb,
        action_in,
        attn_gain.reshape(1, width),
        mlp_gain.reshape(1, width),
        final_gain.reshape(1, width),
        head_w,
    )


def unpack_first(got, cols):
    rows, total = got[0].shape
    count = len(got)

    def kernel(*refs):
        qa, kv = refs[count:]
        for r in range(count):
            qa[r * rows : (r + 1) * rows] = refs[r][:, :cols]
            kv[r * rows : (r + 1) * rows] = refs[r][:, cols:]

    return pl.pallas_call(
        kernel,
        out_shape=(like(count * rows, cols), like(count * rows, total - cols)),
        name="unpack_first",
        compiler_params=grant(8),
    )(*got)


def queries(an, own, other, heads_cols, scale, span):
    mid, cols = own.shape

    def kernel(a, w0, w1, *refs):
        outs, total = refs[:-1], refs[-1]
        v = dot(a[:, :mid], w0[...]) + dot(a[:, mid:], w1[...])
        total[:, :heads_cols] = v[:, :heads_cols] * scale
        total[:, heads_cols:] = v[:, heads_cols:]
        split_rows(total[...], span, outs)

    return pl.pallas_call(
        kernel,
        out_shape=[like(span, cols) for _ in RELS],
        scratch_shapes=[pltpu.VMEM((an.shape[0], cols), F32)],
        name="queries",
        compiler_params=grant(8),
    )(an, own, other)


def normed_blocks(prefix, gain):
    positions, width = prefix.shape
    step, count = 256, 16
    per, no = width // 16, 4

    def kernel(x, g, out):
        oo, ii, cc = (lax.axis_index(n) for n in ("o", "i", "c"))
        v = x[...].astype(F32)
        scale = lax.rsqrt(jnp.mean(v * v, axis=-1, keepdims=True) + 1e-06)
        for b in range(count):
            r, i, c = b % no, (b // no) % 2, b // (2 * no)
            block = ((oo ^ r) * 2 + (cc ^ c)) * 2 + (ii ^ i)
            src = pl.ds(pl.multiple_of(block * per, per), per)
            out[:, b * per : (b + 1) * per] = (x[:, src].astype(F32) * scale * g[:, src]).astype(BF)

    return pl.pallas_call(
        kernel,
        grid=(positions // step,),
        out_shape=like(positions, width),
        in_specs=[pl.BlockSpec((step, width), lambda s: (s, 0)), at(1, width)],
        out_specs=pl.BlockSpec((step, width), lambda s: (s, 0)),
        name="normed_blocks",
        compiler_params=grant(16),
    )(prefix, gain.reshape(1, width))


def attention(prefix, kv_own, kv_oth, qa, length, heads_cols):
    positions, width = prefix.shape
    tall, hd = kv_own[0].shape
    span, qa_cols = qa[0].shape
    per_part = heads_cols // hd
    heads = len(RELS) * per_part
    step = 512
    steps = positions // step

    def kernel(len_ref, pn, *refs):
        own, oth, qs = refs[0:4], refs[4:8], refs[8:12]
        outs = refs[12:16]
        q_all, acc, den = refs[16:19]
        s = pl.program_id(0)
        ii, xx = lax.axis_index("i"), lax.axis_index("x")

        @pl.when(s == 0)
        def _():
            q_all[...] = jnp.zeros_like(q_all)
            for k in range(len(RELS)):
                for h in range(per_part):
                    q_all[PAD * (k * per_part + h) : PAD * (k * per_part + h) + span] = qs[k][
                        :, h * hd : (h + 1) * hd
                    ]
            acc[...] = jnp.zeros_like(acc)
            den[...] = jnp.zeros_like(den)

        same = diff = 0.0
        for c, refs_c in enumerate((own, oth)):
            for i in range(2):
                m = pn[:, (c * 2 + i) * tall : (c * 2 + i + 1) * tall]
                same = same + dot(m, refs_c[i][...])
                diff = diff + dot(m, refs_c[2 + i][...])
        first = xx == 0
        same, diff = same.astype(BF), diff.astype(BF)
        keys = jnp.where(first, same, diff)
        vals = jnp.where(first, diff, same)
        nt = (((1,), (1,)), ((), ()))
        sc = lax.dot_general(q_all[...], keys, nt, preferred_element_type=F32)
        spot = s * step + lax.broadcasted_iota(jnp.int32, sc.shape, 1)
        p = jnp.where(spot < len_ref[lax.axis_index("x") * 2 + lax.axis_index("c")], jnp.exp(sc), 0.0)
        den[...] += jnp.sum(p, axis=-1, keepdims=True)
        acc[...] += dot(p.astype(BF), vals)

        @pl.when(s == steps - 1)
        def _():
            parts = [q[:, heads_cols:] for q in qs]
            flat = ii == 0
            lo = [jnp.where(flat, parts[2 * k], parts[2 * k + 1]) for k in range(2)]
            hi = [jnp.where(flat, parts[2 * k + 1], parts[2 * k]) for k in range(2)]
            sa = jnp.concatenate([lo[0], hi[0]], axis=1)
            da = jnp.concatenate([lo[1], hi[1]], axis=1)
            ak, av = jnp.where(first, sa, da), jnp.where(first, da, sa)
            pa = jnp.exp(lax.dot_general(q_all[...], ak, nt, preferred_element_type=F32))
            total = den[...] + jnp.sum(pa, axis=-1, keepdims=True)
            res = ((acc[...] + dot(pa.astype(BF), av)) / total).astype(BF)
            for k in range(len(RELS)):
                for h in range(per_part):
                    n = PAD * (k * per_part + h)
                    outs[k][:, h * hd : (h + 1) * hd] = res[n : n + span]

    return pl.pallas_call(
        kernel,
        grid=(steps,),
        out_shape=[like(span, heads_cols) for _ in RELS],
        in_specs=[
            pl.BlockSpec(memory_space=pltpu.SMEM),
            pl.BlockSpec((step, width), lambda s: (s, 0)),
        ]
        + [at(tall, hd)] * 8
        + [at(span, qa_cols)] * 4,
        out_specs=[at(span, heads_cols)] * 4,
        scratch_shapes=[
            pltpu.VMEM((PAD * heads, hd), BF),
            pltpu.VMEM((PAD * heads, hd), F32),
            pltpu.VMEM((PAD * heads, 1), F32),
        ],
        name="prefix_attention",
        compiler_params=grant(24),
    )(length, prefix, *kv_own, *kv_oth, *qa)


def row_outs(rows, width, parts):
    return [like(rows, width, dtype=F32)] + [like(rows, width) for _ in range(parts - 1)]


def out_project(attn, pieces, units):
    rows = attn[0].shape[0]
    parts, count = len(attn), len(pieces)
    tall, cols = pieces[0].shape
    place = tall // units - 1

    def kernel(*refs):
        a_refs, w_refs = refs[:parts], refs[parts : parts + count]
        outs, a_all, total = refs[parts + count : -2], refs[-2], refs[-1]
        for k in range(parts):
            a_all[PAD * k : PAD * k + rows] = a_refs[k][...]
        for b in range(0, count, 2):
            pair = jnp.concatenate([w_refs[b][...], w_refs[b + 1][...]], axis=1)
            total[:, b * cols : (b + 2) * cols] = dot(a_all[...], pair)
        split_rows(total, rows, outs)

    return pl.pallas_call(
        kernel,
        grid=(1,),
        out_shape=row_outs(rows, count * cols, parts),
        in_specs=[at(rows, units)] * parts
        + [pl.BlockSpec((units, cols), lambda s: (place, 0))] * count,
        out_specs=[at(rows, count * cols)] * parts,
        scratch_shapes=[
            pltpu.VMEM((PAD * parts, units), BF),
            pltpu.VMEM((PAD * parts, count * cols), F32),
        ],
        name="out_project",
        compiler_params=grant(12),
    )(*attn, *pieces)


def feed_forward(mn, gu, od, units):
    rows = mn[0].shape[0]
    parts, count = len(mn), len(gu)
    per, cols = gu[0].shape[0], od[0].shape[1]
    step = 256
    steps = units // step

    def kernel(*refs):
        m_refs, refs = refs[:parts], refs[parts:]
        g_refs, u_refs, d_refs = refs[:count], refs[count : 2 * count], refs[2 * count : 3 * count]
        outs, m_all, total = refs[3 * count : -2], refs[-2], refs[-1]
        s = pl.program_id(0)

        @pl.when(s == 0)
        def _():
            for k in range(parts):
                m_all[PAD * k : PAD * k + rows] = m_refs[k][...]
            total[...] = jnp.zeros_like(total)

        gate = dot(m_all[...], jnp.concatenate([g[...] for g in g_refs], axis=0))
        up = dot(m_all[...], jnp.concatenate([u[...] for u in u_refs], axis=0))
        hid = (jax.nn.gelu(gate, approximate=True) * up).astype(BF)
        for b in range(0, count, 2):
            pair = jnp.concatenate([d_refs[b][...], d_refs[b + 1][...]], axis=1)
            total[:, b * cols : (b + 2) * cols] += dot(hid, pair)

        @pl.when(s == steps - 1)
        def _():
            split_rows(total, rows, outs)

    return pl.pallas_call(
        kernel,
        grid=(steps,),
        out_shape=row_outs(rows, count * cols, parts),
        in_specs=[at(rows, count * per)] * parts
        + [pl.BlockSpec((per, step), lambda s: (0, s))] * count
        + [pl.BlockSpec((per, step), lambda s: (0, s + steps))] * count
        + [pl.BlockSpec((step, cols), lambda s: (s, 0))] * count,
        out_specs=[at(rows, count * cols)] * parts,
        scratch_shapes=[
            pltpu.VMEM((PAD * parts, count * per), BF),
            pltpu.VMEM((PAD * parts, count * cols), F32),
        ],
        name="feed_forward",
        compiler_params=grant(20),
    )(*mn, *gu, *gu, *od)


def velocity_and_loss(h1, parts, gains, head_p, noise, actions):
    rows, _ = h1.shape
    adim = head_p.shape[0]
    nt = (((1,), (1,)), ((), ()))

    def kernel(h, *refs):
        p_refs, (g, w, nz, ac, vel, loss) = refs[: len(parts)], refs[len(parts) :]
        at_own = lax.axis_index("x") * 2 + lax.axis_index("c")
        v = h[...]
        for p in p_refs:
            v = v + p[...].astype(F32)
        v = v * lax.rsqrt(jnp.mean(v * v, axis=-1, keepdims=True) + 1e-06) * g[1:2, :]
        out = lax.dot_general(w[...], v.astype(BF), nt, preferred_element_type=F32)
        vel[...] = out
        diff = out - (nz[at_own] - ac[at_own])
        square = jnp.sum(diff * diff, axis=1, keepdims=True)
        loss[...] = jnp.sum(square, axis=0, keepdims=True) / (rows * adim)

    return pl.pallas_call(
        kernel,
        out_shape=(like(adim, rows, dtype=F32), like(1, 1, dtype=F32)),
        name="velocity_and_loss",
        compiler_params=grant(8),
    )(h1, *parts, gains, head_p, noise, actions)


def make(no, ni, nx, nc):
    def flip(value, axis):
        return lax.ppermute(value, axis, [(0, 1), (1, 0)])

    def cross(value, di, dx):
        pairs = [
            (i * nx + x, (i ^ di) * nx + (x ^ dx)) for i in range(ni) for x in range(nx)
        ]
        return lax.ppermute(value, ("i", "x"), pairs)

    def spread(value):
        return [value] + [cross(value, di, dx) for di, dx in RELS[1:]]

    def exchange(parts):
        return [parts[0]] + [cross(p, di, dx) for p, (di, dx) in zip(parts[1:], RELS[1:])]

    def turned(value, r):
        return lax.ppermute(
            value,
            ("o", "i", "c"),
            [
                ((o * ni + i) * nc + c, ((o ^ r) * ni + c) * nc + i)
                for o in range(no)
                for i in range(ni)
                for c in range(nc)
            ],
        )

    def hop(value, pairs):
        return lax.ppermute(value, "o", pairs)

    def partner(r):
        return [(o, o ^ r) for o in range(no)]

    MIDDLE, OUTWARD = [(1, 2), (2, 1)], [(1, 0), (2, 3)]

    def fast(
        prefix_hidden,
        prefix_len,
        actions,
        noise,
        time_index,
        prefix_gain,
        key_weight,
        value_weight,
        action_in,
        attn_gain,
        query_w,
        akey_w,
        avalue_w,
        out_w,
        mlp_gain,
        gate_w,
        up_w,
        down_w,
        final_gain,
        head_w,
):
        own_eps, positions, width = prefix_hidden.shape
        _, span, adim = actions.shape
        expert = action_in.shape[1]
        hd = key_weight.shape[1]
        heads_cols = query_w.shape[1]
        units = gate_w.shape[1]
        oo, xx, cc = (lax.axis_index(a) for a in ("o", "x", "c"))

        def order(first, second, at_one):
            return jnp.where(at_one == 0, first, second), jnp.where(at_one == 0, second, first)

        first, gu = pack_weights(
            query_w, akey_w, avalue_w, key_weight, value_weight, gate_w, up_w
        )
        got = [turned(first, r) for r in range(no)]
        gu_0 = turned(gu, 0)
        out_0 = turned(out_w, 0)
        down_0 = turned(down_w, 0)

        times = (time_index.astype(F32) + 0.5) / TSTEPS
        x_t = times[:, None, None] * noise + (1.0 - times)[:, None, None] * actions
        x_in = x_t.astype(BF)

        def mine_of(values):
            v = values.reshape((nx, nc) + values.shape[1:])
            return lax.dynamic_index_in_dim(v, cc, 1, keepdims=False)

        packed = jnp.concatenate(
            [
                mine_of(x_in).astype(F32),
                jnp.broadcast_to(mine_of(times)[:, None, None], (nx, 1, adim)),
            ],
            axis=1,
        )
        packed_oth = flip(packed, "i")
        a0, a1 = order(packed[0], packed[1], xx)
        b0, b1 = order(packed_oth[0], packed_oth[1], xx)
        packed = jnp.stack([a0, b0, a1, b1])
        temb = time_embed(packed[:, span, 0], expert)
        x_g = jnp.pad(packed[:, :span], ((0, 0), (0, PAD - span), (0, 0))).astype(BF)
        an, h0, gains, head_p = expert_in(
            x_g.reshape(len(RELS) * PAD, adim),
            temb,
            action_in,
            attn_gain,
            mlp_gain,
            final_gain,
            head_w.T,
            span,
            expert // (no * nc),
        )

        got = [after(t, an) for t in got]
        gu_t = after(gu_0, *got)
        gu_a, gu_b = hop(gu_t, partner(1)), hop(gu_t, MIDDLE)
        qa_own, kv = unpack_first(got, first.shape[1] - hd)
        kv_all = spread(kv)
        out_t = after(out_0, qa_own)
        out_got = [out_t] + [hop(out_t, partner(r)) for r in range(1, no)]
        qa_oth = flip(qa_own, "c")
        q_parts = queries(an, qa_own, qa_oth, heads_cols, hd ** (-0.5), span)
        qa = exchange(q_parts)
        pn = normed_blocks(
            after(prefix_hidden, q_parts[0]).reshape(positions, width), prefix_gain
        )
        gu_c, gu_d = hop(after(gu_b, q_parts[0]), OUTWARD), hop(after(gu_a, q_parts[0]), MIDDLE)
        down_t = after(down_0, q_parts[0])
        down_got = [down_t] + [hop(down_t, partner(r)) for r in range(1, no)]
        kv_all = [after(t, pn) for t in kv_all]
        kv_oth = [flip(t, "c") for t in kv_all]
        attn = attention(pn, kv_all, kv_oth, qa, prefix_len, heads_cols)

        attn_in = exchange(attn)
        gu_e = hop(after(gu_d, attn[0]), OUTWARD)
        out_all = out_got + [flip(after(t, pn), "c") for t in out_got]
        out_parts = out_project(attn_in, out_all, heads_cols)
        out_in = exchange(out_parts)
        h1 = h0 + sum(t.astype(F32) for t in out_in)

        mn = spread(rms(h1, gains[0]).astype(BF))
        inner = (oo == 1) | (oo == 2)
        gu_t, gu_a, gu_b, gu_c, gu_d = (
            after(t, out_parts[0]) for t in (gu_t, gu_a, gu_b, gu_c, gu_d)
        )
        gu_e = after(gu_e, *mn)
        gu_got = [gu_t, gu_a, jnp.where(inner, gu_d, gu_c), jnp.where(inner, gu_b, gu_e)]
        gu_all = gu_got + [flip(t, "c") for t in gu_got]
        down_got = [after(t, *mn) for t in down_got]
        down_all = down_got + [flip(t, "c") for t in down_got]
        ff_parts = feed_forward(mn, gu_all, down_all, units)
        ff_in = exchange(ff_parts)
        velocity, loss = velocity_and_loss(
            h1, ff_in, gains, head_p, noise.transpose(0, 2, 1), actions.transpose(0, 2, 1)
        )
        velocity = velocity.reshape(own_eps, adim, span).transpose(0, 2, 1)
        return velocity, loss.reshape(own_eps)

    def on_device(*values):
        eps, positions, _ = values[0].shape
        expert = values[8].shape[1]
        fits = (
            (no, ni, nx, nc) == (4, 2, 2, 2)
            and eps == 1
            and values[2].shape[1] <= PAD
            and positions % 256 == 0
            and (expert // (no * nc)) % LANES == 0
            and values[6].shape[0] == 2 * values[10].shape[0] == 2 * values[13].shape[1]
        )
        if not fits:
            return gather_all(*values)
        return fast(*values)

    return on_device


def solution(mesh):
    in_specs = (
        P(("dp", "mp"), None, None),
        P("dp"),
        P("dp", None, None),
        P("dp", None, None),
        P("dp"),
        P(),
        P("dp", None),
        P("dp", None),
        P(),
        P(),
        P("dp", "mp"),
        P("dp", None),
        P("dp", None),
        P("mp", "dp"),
        P(),
        P("dp", "mp"),
        P("dp", "mp"),
        P("mp", "dp"),
        P(),
        P(),
    )
    out_specs = (P(("dp", "mp"), None, None), P(("dp", "mp")))
    ndp, nmp = mesh.shape["dp"], mesh.shape["mp"]
    sizes = (ndp // 2, 2, nmp // 2, 2)
    fine = Mesh(mesh.devices.reshape(sizes), DP + MP)
    names = {"dp": DP, "mp": MP}

    def finer(spec):
        flat = []
        for entry in spec:
            entry = (entry,) if isinstance(entry, str) else entry
            flat.append(None if entry is None else tuple(n for e in entry for n in names[e]))
        return P(*flat)

    return jax.shard_map(
        make(*sizes),
        mesh=fine,
        in_specs=tuple(finer(s) for s in in_specs),
        out_specs=tuple(finer(s) for s in out_specs),
        check_vma=False,
    )
```

```python
import math

import jax
import jax.numpy as jnp
from jax import lax
from jax.experimental import pallas as pl
from jax.experimental.pallas import tpu as pltpu
from jax.sharding import Mesh
from jax.sharding import PartitionSpec as P


TSTEPS = 1000
BF = jnp.bfloat16
F32 = jnp.float32
LANES = 128
PAD = 64
DP, MP = ("o", "i"), ("x", "c")
RELS = ((0, 0), (1, 0), (0, 1), (1, 1))


def rms(values, gain):
    return values * lax.rsqrt(jnp.mean(values * values, axis=-1, keepdims=True) + 1e-06) * gain


def time_embed(times, width):
    half = width // 2
    steps = jnp.arange(half, dtype=jnp.float32)
    period = 0.004 * jnp.power(jnp.float32(1000.0), steps / (half - 1))
    angle = times[:, None] * (2.0 * math.pi) / period[None, :]
    return jnp.concatenate([jnp.sin(angle), jnp.cos(angle)], axis=-1)


def attend(query, pkeys, pvals, akeys, avals, lengths):
    live = jnp.arange(pkeys.shape[1], dtype=jnp.int32)[None, :] < lengths[:, None]
    scores = jnp.einsum("erd,epd->erp", query, pkeys, preferred_element_type=jnp.float32)
    probs = jnp.where(live[:, None, :], jnp.exp(scores), 0.0)
    action_scores = jnp.einsum("erd,ecd->erc", query, akeys, preferred_element_type=jnp.float32)
    action_probs = jnp.exp(action_scores)
    denom = jnp.sum(probs, axis=-1) + jnp.sum(action_probs, axis=-1)
    weighted = jnp.einsum(
        "erp,epd->erd", probs.astype(jnp.bfloat16), pvals, preferred_element_type=jnp.float32
    )
    weighted = weighted + jnp.einsum(
        "erc,ecd->erd", action_probs.astype(jnp.bfloat16), avals, preferred_element_type=jnp.float32
    )
    return (weighted / denom[:, :, None]).astype(jnp.bfloat16)


def gather_all(
    prefix_hidden,
    prefix_len,
    actions,
    noise,
    time_index,
    prefix_gain,
    key_weight,
    value_weight,
    action_in,
    attn_gain,
    query_w,
    akey_w,
    avalue_w,
    out_w,
    mlp_gain,
    gate_w,
    up_w,
    down_w,
    final_gain,
    head_w,
):
    own_eps, positions, width = prefix_hidden.shape
    group_eps, span, adim = actions.shape
    expert = action_in.shape[1]
    head_size = key_weight.shape[1]
    local_heads = query_w.shape[1] // head_size
    rows_total = group_eps * span
    own_rows = own_eps * span
    member = lax.axis_index(MP)
    first_row = member * own_rows
    first_ep = member * own_eps
    times = (time_index.astype(jnp.float32) + 0.5) / TSTEPS
    x_t = times[:, None, None] * noise + (1.0 - times)[:, None, None] * actions
    target = noise - actions
    x_in = x_t.reshape(rows_total, adim).astype(jnp.bfloat16)
    temb = time_embed(times, expert)
    h0 = (
        jnp.dot(x_in, action_in, preferred_element_type=jnp.float32).reshape(
            group_eps, span, expert
        )
        + temb[:, None, :]
    )
    h0 = h0.reshape(rows_total, expert)
    key_full, value_full = (
        lax.all_gather(key_weight, DP, axis=0, tiled=True),
        lax.all_gather(value_weight, DP, axis=0, tiled=True),
    )
    prefix_normed = rms(
        prefix_hidden.reshape(own_eps * positions, width).astype(jnp.float32), prefix_gain
    ).astype(jnp.bfloat16)
    pkeys = (
        jnp.dot(prefix_normed, key_full, preferred_element_type=jnp.float32)
        .astype(jnp.bfloat16)
        .reshape(own_eps, positions, head_size)
    )
    pvals = (
        jnp.dot(prefix_normed, value_full, preferred_element_type=jnp.float32)
        .astype(jnp.bfloat16)
        .reshape(own_eps, positions, head_size)
    )
    normed = rms(h0, attn_gain).astype(jnp.bfloat16)
    query_full, akey_full, avalue_full = (
        lax.all_gather(query_w, DP, axis=0, tiled=True),
        lax.all_gather(akey_w, DP, axis=0, tiled=True),
        lax.all_gather(avalue_w, DP, axis=0, tiled=True),
    )
    query = (
        jnp.dot(normed, query_full, preferred_element_type=jnp.float32) * head_size ** (-0.5)
    ).astype(jnp.bfloat16)
    akeys = (
        jnp.dot(normed, akey_full, preferred_element_type=jnp.float32)
        .astype(jnp.bfloat16)
        .reshape(group_eps, span, head_size)
    )
    avals = (
        jnp.dot(normed, avalue_full, preferred_element_type=jnp.float32)
        .astype(jnp.bfloat16)
        .reshape(group_eps, span, head_size)
    )
    keys_all, vals_all = (
        lax.all_gather(pkeys, MP, axis=0, tiled=True),
        lax.all_gather(pvals, MP, axis=0, tiled=True),
    )
    attn = attend(
        query.reshape(group_eps, span * local_heads, head_size),
        keys_all,
        vals_all,
        akeys,
        avals,
        prefix_len,
    )
    attn = attn.reshape(rows_total, local_heads * head_size)
    out_full = lax.all_gather(out_w, DP, axis=1, tiled=True)
    gate_full, up_full = (
        lax.all_gather(gate_w, DP, axis=0, tiled=True),
        lax.all_gather(up_w, DP, axis=0, tiled=True),
    )
    down_full = lax.all_gather(down_w, DP, axis=1, tiled=True)
    h0_own = lax.dynamic_slice_in_dim(h0, first_row, own_rows, 0)
    h1 = h0_own + lax.psum_scatter(
        jnp.dot(attn, out_full, preferred_element_type=jnp.float32).astype(jnp.bfloat16),
        MP,
        scatter_dimension=0,
        tiled=True,
    ).astype(jnp.float32)
    mixed_own = rms(h1, mlp_gain).astype(jnp.bfloat16)
    mixed = lax.all_gather(mixed_own, MP, axis=0, tiled=True)
    gate = jnp.dot(mixed, gate_full, preferred_element_type=jnp.float32)
    upper = jnp.dot(mixed, up_full, preferred_element_type=jnp.float32)
    hidden = (jax.nn.gelu(gate, approximate=True) * upper).astype(jnp.bfloat16)
    h2 = h1 + lax.psum_scatter(
        jnp.dot(hidden, down_full, preferred_element_type=jnp.float32).astype(jnp.bfloat16),
        MP,
        scatter_dimension=0,
        tiled=True,
    ).astype(jnp.float32)
    final = rms(h2, final_gain).astype(jnp.bfloat16)
    velocity = jnp.dot(final, head_w, preferred_element_type=jnp.float32).reshape(
        own_eps, span, adim
    )
    own_target = lax.dynamic_slice_in_dim(target, first_ep, own_eps, 0)
    diff = velocity - own_target
    ep_loss = jnp.mean(diff * diff, axis=(1, 2))
    return (velocity, ep_loss)


def dot(a, b):
    return jnp.dot(a, b, preferred_element_type=F32)


def after(values, *earlier):
    return lax.optimization_barrier((values,) + earlier)[0]


def at(*block):
    return pl.BlockSpec(block, lambda *s: (0,) * len(block))


def grant(mib):
    return pltpu.CompilerParams(vmem_limit_bytes=mib * 2**20)


def like(*shape, dtype=BF):
    return jax.ShapeDtypeStruct(shape, dtype)


def split_rows(total, rows, outs):
    outs[0][...] = total[:rows].astype(outs[0].dtype)
    for k in range(1, len(outs)):
        outs[k][...] = total[PAD * k : PAD * k + rows].astype(outs[k].dtype)


def pack_weights(query_w, akey_w, avalue_w, key_w, value_w, gate_w, up_w):
    rows, hq = query_w.shape
    ha, hk = akey_w.shape[1], key_w.shape[1]
    quarter, half = ha // 2, key_w.shape[0] // 2
    units = gate_w.shape[1]

    def kernel(q, ak, av, kw, vw, gw, uw, first, gu):
        xx, cc = lax.axis_index("x"), lax.axis_index("c")
        cols = pl.ds(pl.multiple_of(cc * quarter, quarter), quarter)
        part = pl.ds(pl.multiple_of(cc * half, half), half)
        first[:, :hq] = q[...]

        @pl.when(xx == 0)
        def _():
            first[:, hq : hq + quarter] = ak[:, cols]
            first[:, hq + quarter :] = kw[part, :]

        @pl.when(xx != 0)
        def _():
            first[:, hq : hq + quarter] = av[:, cols]
            first[:, hq + quarter :] = vw[part, :]

        gu[:, :units] = gw[...]
        gu[:, units:] = uw[...]

    return pl.pallas_call(
        kernel,
        out_shape=(
            like(rows, hq + quarter + hk),
            like(rows, 2 * units),
        ),
        name="pack_weights",
    )(query_w, akey_w, avalue_w, key_w, value_w, gate_w, up_w)


def expert_in(x_g, temb, action_in, attn_gain, mlp_gain, final_gain, head_w, span, per):
    rows = x_g.shape[0]
    groups, width = temb.shape
    adim = head_w.shape[0]
    count = width // per

    def kernel(x, te, act, ga, gm, gf, hw, an, h0, gains, head_p, h_all):
        oo, cc = lax.axis_index("o"), lax.axis_index("c")
        for b in range(count):
            r, c = b % (count // 2), b // (count // 2)
            block = (oo ^ r) * 2 + (cc ^ c)
            src = pl.ds(pl.multiple_of(block * per, per), per)
            dst = slice(b * per, (b + 1) * per)
            h = dot(x[...], act[:, src])
            for k in range(groups):
                h_all[PAD * k : PAD * (k + 1), dst] = h[PAD * k : PAD * (k + 1)] + te[k : k + 1, src]
            gains[0:1, dst] = gm[:, src]
            gains[1:2, dst] = gf[:, src]
            gains[2:3, dst] = ga[:, src]
            head_p[:, dst] = hw[:, src]
        h = h_all[...]
        h0[...] = h[:span]
        an[...] = (
            h * lax.rsqrt(jnp.mean(h * h, axis=-1, keepdims=True) + 1e-06) * gains[2:3, :]
        ).astype(BF)

    return pl.pallas_call(
        kernel,
        out_shape=(
            like(rows, width),
            like(span, width, dtype=F32),
            like(8, width, dtype=F32),
            like(adim, width),
        ),
        scratch_shapes=[pltpu.VMEM((rows, width), F32)],
        name="expert_in",
    )(
        x_g,
        temb,
        action_in,
        attn_gain.reshape(1, width),
        mlp_gain.reshape(1, width),
        final_gain.reshape(1, width),
        head_w,
    )


def unpack_first(got, cols):
    rows, total = got[0].shape
    count = len(got)

    def kernel(*refs):
        qa, kv = refs[count:]
        for r in range(count):
            qa[r * rows : (r + 1) * rows] = refs[r][:, :cols]
            kv[r * rows : (r + 1) * rows] = refs[r][:, cols:]

    return pl.pallas_call(
        kernel,
        out_shape=(like(count * rows, cols), like(count * rows, total - cols)),
        name="unpack_first",
        compiler_params=grant(8),
    )(*got)


def queries(an, own, other, heads_cols, scale, span):
    mid, cols = own.shape

    def kernel(a, w0, w1, *refs):
        outs, total = refs[:-1], refs[-1]
        v = dot(a[:, :mid], w0[...]) + dot(a[:, mid:], w1[...])
        total[:, :heads_cols] = v[:, :heads_cols] * scale
        total[:, heads_cols:] = v[:, heads_cols:]
        split_rows(total[...], span, outs)

    return pl.pallas_call(
        kernel,
        out_shape=[like(span, cols) for _ in RELS],
        scratch_shapes=[pltpu.VMEM((an.shape[0], cols), F32)],
        name="queries",
        compiler_params=grant(8),
    )(an, own, other)


def attention(prefix, gain, kv_own, kv_oth, qa, length, heads_cols):
    positions, width = prefix.shape
    tall, hd = kv_own[0].shape
    span, _ = qa[0].shape
    per_part = heads_cols // hd
    heads = len(RELS) * per_part
    step = 512 if positions % 512 == 0 else 256
    steps = positions // step
    count = 16
    per, no = width // count, count // 4

    def kernel(len_ref, x_hbm, g, *refs):
        own, oth, qs = refs[0:4], refs[4:8], refs[8:12]
        outs = refs[12:16]
        x_all, q_all, pn, sems = refs[16:20]
        oo, ii, xx, cc = (lax.axis_index(n) for n in ("o", "i", "x", "c"))
        copies = [
            pltpu.make_async_copy(
                x_hbm.at[s * step : (s + 1) * step], x_all.at[s * step : (s + 1) * step], sems.at[s]
            )
            for s in range(steps)
        ]
        for copy in copies:
            copy.start()
        q_all[...] = jnp.zeros_like(q_all)
        for k in range(len(RELS)):
            for h in range(per_part):
                n = PAD * (k * per_part + h)
                q_all[n : n + span] = qs[k][:, h * hd : (h + 1) * hd]
        first = xx == 0
        nt = (((1,), (1,)), ((), ()))
        parts = [q[:, heads_cols:] for q in qs]
        flat = ii == 0
        lo = [jnp.where(flat, parts[2 * k], parts[2 * k + 1]) for k in range(2)]
        hi = [jnp.where(flat, parts[2 * k + 1], parts[2 * k]) for k in range(2)]
        sa = jnp.concatenate([lo[0], hi[0]], axis=1)
        da = jnp.concatenate([lo[1], hi[1]], axis=1)
        ak, av = jnp.where(first, sa, da), jnp.where(first, da, sa)
        pa = jnp.exp(lax.dot_general(q_all[...], ak, nt, preferred_element_type=F32))
        den = jnp.sum(pa, axis=-1, keepdims=True)
        acc = dot(pa.astype(BF), av)
        limit = len_ref[xx * 2 + cc]
        for s in range(steps):
            copies[s].wait()
            x = x_all.at[s * step : (s + 1) * step]
            v = x[...].astype(F32)
            scale = lax.rsqrt(jnp.mean(v * v, axis=-1, keepdims=True) + 1e-06)
            for b in range(count):
                r, i, c = b % no, (b // no) % 2, b // (2 * no)
                block = ((oo ^ r) * 2 + (cc ^ c)) * 2 + (ii ^ i)
                src = pl.ds(pl.multiple_of(block * per, per), per)
                pn[:, b * per : (b + 1) * per] = (x[:, src].astype(F32) * scale * g[:, src]).astype(BF)
            same = diff = 0.0
            for c, refs_c in enumerate((own, oth)):
                for i in range(2):
                    m = pn[:, (c * 2 + i) * tall : (c * 2 + i + 1) * tall]
                    same = same + dot(m, refs_c[i][...])
                    diff = diff + dot(m, refs_c[2 + i][...])
            same, diff = same.astype(BF), diff.astype(BF)
            keys = jnp.where(first, same, diff)
            vals = jnp.where(first, diff, same)
            sc = lax.dot_general(q_all[...], keys, nt, preferred_element_type=F32)
            spot = s * step + lax.broadcasted_iota(jnp.int32, sc.shape, 1)
            p = jnp.where(spot < limit, jnp.exp(sc), 0.0)
            den = den + jnp.sum(p, axis=-1, keepdims=True)
            acc = acc + dot(p.astype(BF), vals)
        res = (acc / den).astype(BF)
        for k in range(len(RELS)):
            for h in range(per_part):
                n = PAD * (k * per_part + h)
                outs[k][:, h * hd : (h + 1) * hd] = res[n : n + span]

    vmem = pl.BlockSpec(memory_space=pltpu.VMEM)
    return pl.pallas_call(
        kernel,
        out_shape=[like(span, heads_cols) for _ in RELS],
        in_specs=[pl.BlockSpec(memory_space=pltpu.SMEM), pl.BlockSpec(memory_space=pltpu.HBM)]
        + [vmem] * 13,
        out_specs=[vmem] * 4,
        scratch_shapes=[
            pltpu.VMEM((positions, width), BF),
            pltpu.VMEM((PAD * heads, hd), BF),
            pltpu.VMEM((step, width), BF),
            pltpu.SemaphoreType.DMA((steps,)),
        ],
        name="prefix_attention",
        compiler_params=grant(28),
    )(length, prefix, gain.reshape(1, width), *kv_own, *kv_oth, *qa)


def row_outs(rows, width, parts):
    return [like(rows, width, dtype=F32)] + [like(rows, width) for _ in range(parts - 1)]


def out_project(attn, pieces, units):
    rows = attn[0].shape[0]
    parts, count = len(attn), len(pieces)
    tall, cols = pieces[0].shape
    place = tall // units - 1

    def kernel(*refs):
        a_refs, w_refs = refs[:parts], refs[parts : parts + count]
        outs, a_all, total = refs[parts + count : -2], refs[-2], refs[-1]
        for k in range(parts):
            a_all[PAD * k : PAD * k + rows] = a_refs[k][...]
        for b in range(0, count, 2):
            pair = jnp.concatenate([w_refs[b][...], w_refs[b + 1][...]], axis=1)
            total[:, b * cols : (b + 2) * cols] = dot(a_all[...], pair)
        split_rows(total, rows, outs)

    return pl.pallas_call(
        kernel,
        grid=(1,),
        out_shape=row_outs(rows, count * cols, parts),
        in_specs=[at(rows, units)] * parts
        + [pl.BlockSpec((units, cols), lambda s: (place, 0))] * count,
        out_specs=[at(rows, count * cols)] * parts,
        scratch_shapes=[
            pltpu.VMEM((PAD * parts, units), BF),
            pltpu.VMEM((PAD * parts, count * cols), F32),
        ],
        name="out_project",
        compiler_params=grant(12),
    )(*attn, *pieces)


def feed_forward(mn, gu_own, gu_oth, down, units):
    rows, parts = mn[0].shape[0], len(mn)
    count, per, cols = len(down), gu_own[0].shape[0], down[0].shape[1]
    step = 256

    def kernel(*refs):
        m_refs, refs = refs[:parts], refs[parts:]
        own, oth, d_refs = refs[:6], refs[6:12], refs[12 : 12 + count]
        outs, m_all = refs[12 + count : -1], refs[-1]
        oo = lax.axis_index("o")
        inner = (oo == 1) | (oo == 2)
        for k in range(parts):
            m_all[PAD * k : PAD * k + rows] = m_refs[k][...]
        m = m_all[...]

        def stacked(u):
            blocks = []
            for t, a, b, c, d, e in (own, oth):
                t, a, b, c, d, e = (w[:, u : u + step] for w in (t, a, b, c, d, e))
                blocks += [t, a, jnp.where(inner, d, c), jnp.where(inner, b, e)]
            return jnp.concatenate(blocks, axis=0)

        hid = []
        for u in range(0, units, step):
            gate, up = dot(m, stacked(u)), dot(m, stacked(units + u))
            hid.append((jax.nn.gelu(gate, approximate=True) * up).astype(BF))
        hid = jnp.concatenate(hid, axis=1)
        for b in range(0, count, 2):
            total = dot(hid, jnp.concatenate([d_refs[b][...], d_refs[b + 1][...]], axis=1))
            for k in range(parts):
                part = total[PAD * k : PAD * k + rows]
                outs[k][:, b * cols : (b + 2) * cols] = part.astype(outs[k].dtype)

    return pl.pallas_call(
        kernel,
        out_shape=row_outs(rows, count * cols, parts),
        scratch_shapes=[pltpu.VMEM((PAD * parts, count * per), BF)],
        name="feed_forward",
        compiler_params=grant(24),
    )(*mn, *gu_own, *gu_oth, *down)


def velocity_and_loss(h1, parts, gains, head_p, noise, actions):
    rows, _ = h1.shape
    adim = head_p.shape[0]
    nt = (((1,), (1,)), ((), ()))

    def kernel(h, *refs):
        p_refs, (g, w, nz, ac, vel, loss) = refs[: len(parts)], refs[len(parts) :]
        at_own = lax.axis_index("x") * 2 + lax.axis_index("c")
        v = h[...]
        for p in p_refs:
            v = v + p[...].astype(F32)
        v = v * lax.rsqrt(jnp.mean(v * v, axis=-1, keepdims=True) + 1e-06) * g[1:2, :]
        out = lax.dot_general(w[...], v.astype(BF), nt, preferred_element_type=F32)
        vel[...] = out
        diff = out - (nz[at_own] - ac[at_own])
        square = jnp.sum(diff * diff, axis=1, keepdims=True)
        loss[...] = jnp.sum(square, axis=0, keepdims=True) / (rows * adim)

    return pl.pallas_call(
        kernel,
        out_shape=(like(adim, rows, dtype=F32), like(1, 1, dtype=F32)),
        name="velocity_and_loss",
        compiler_params=grant(8),
    )(h1, *parts, gains, head_p, noise, actions)


def make(no, ni, nx, nc):
    def flip(value, axis):
        return lax.ppermute(value, axis, [(0, 1), (1, 0)])

    def cross(value, di, dx):
        pairs = [
            (i * nx + x, (i ^ di) * nx + (x ^ dx)) for i in range(ni) for x in range(nx)
        ]
        return lax.ppermute(value, ("i", "x"), pairs)

    def spread(value):
        return [value] + [cross(value, di, dx) for di, dx in RELS[1:]]

    def exchange(parts):
        return [parts[0]] + [cross(p, di, dx) for p, (di, dx) in zip(parts[1:], RELS[1:])]

    def turned(value, r):
        return lax.ppermute(
            value,
            ("o", "i", "c"),
            [
                ((o * ni + i) * nc + c, ((o ^ r) * ni + c) * nc + i)
                for o in range(no)
                for i in range(ni)
                for c in range(nc)
            ],
        )

    def hop(value, pairs):
        return lax.ppermute(value, "o", pairs)

    def partner(r):
        return [(o, o ^ r) for o in range(no)]

    MIDDLE, OUTWARD = [(1, 2), (2, 1)], [(1, 0), (2, 3)]

    def fast(
        prefix_hidden,
        prefix_len,
        actions,
        noise,
        time_index,
        prefix_gain,
        key_weight,
        value_weight,
        action_in,
        attn_gain,
        query_w,
        akey_w,
        avalue_w,
        out_w,
        mlp_gain,
        gate_w,
        up_w,
        down_w,
        final_gain,
        head_w,
):
        own_eps, positions, width = prefix_hidden.shape
        _, span, adim = actions.shape
        expert = action_in.shape[1]
        hd = key_weight.shape[1]
        heads_cols = query_w.shape[1]
        units = gate_w.shape[1]
        xx, cc = (lax.axis_index(a) for a in ("x", "c"))

        def order(first, second, at_one):
            return jnp.where(at_one == 0, first, second), jnp.where(at_one == 0, second, first)

        first, gu = pack_weights(
            query_w, akey_w, avalue_w, key_weight, value_weight, gate_w, up_w
        )
        got = [turned(first, r) for r in range(no)]
        gu_0 = turned(gu, 0)
        out_0 = turned(out_w, 0)
        down_0 = turned(down_w, 0)

        times = (time_index.astype(F32) + 0.5) / TSTEPS
        x_t = times[:, None, None] * noise + (1.0 - times)[:, None, None] * actions
        x_in = x_t.astype(BF)

        def mine_of(values):
            v = values.reshape((nx, nc) + values.shape[1:])
            return lax.dynamic_index_in_dim(v, cc, 1, keepdims=False)

        packed = jnp.concatenate(
            [
                mine_of(x_in).astype(F32),
                jnp.broadcast_to(mine_of(times)[:, None, None], (nx, 1, adim)),
            ],
            axis=1,
        )
        packed_oth = flip(packed, "i")
        a0, a1 = order(packed[0], packed[1], xx)
        b0, b1 = order(packed_oth[0], packed_oth[1], xx)
        packed = jnp.stack([a0, b0, a1, b1])
        temb = time_embed(packed[:, span, 0], expert)
        x_g = jnp.pad(packed[:, :span], ((0, 0), (0, PAD - span), (0, 0))).astype(BF)
        an, h0, gains, head_p = expert_in(
            x_g.reshape(len(RELS) * PAD, adim),
            temb,
            action_in,
            attn_gain,
            mlp_gain,
            final_gain,
            head_w.T,
            span,
            expert // (no * nc),
        )

        got = [after(t, an) for t in got]
        gu_t = after(gu_0, *got)
        gu_a, gu_b = hop(gu_t, partner(1)), hop(gu_t, MIDDLE)
        qa_own, kv = unpack_first(got, first.shape[1] - hd)
        kv_all = spread(kv)
        out_t = after(out_0, qa_own)
        out_got = [out_t] + [hop(out_t, partner(r)) for r in range(1, no)]
        qa_oth = flip(qa_own, "c")
        q_parts = queries(an, qa_own, qa_oth, heads_cols, hd ** (-0.5), span)
        qa = exchange(q_parts)
        gu_c, gu_d = hop(after(gu_b, q_parts[0]), OUTWARD), hop(after(gu_a, q_parts[0]), MIDDLE)
        down_t = after(down_0, q_parts[0])
        down_got = [down_t] + [hop(down_t, partner(r)) for r in range(1, no)]
        kv_all = [after(t, *qa) for t in kv_all]
        kv_oth = [flip(t, "c") for t in kv_all]
        attn = attention(
            prefix_hidden.reshape(positions, width),
            prefix_gain,
            kv_all,
            kv_oth,
            qa,
            prefix_len,
            heads_cols,
        )

        attn_in = exchange(attn)
        gu_e = hop(after(gu_d, attn[0]), OUTWARD)
        out_all = out_got + [flip(after(t, attn[0]), "c") for t in out_got]
        gu_early = [after(t, attn[0]) for t in (gu_t, gu_a, gu_b)]
        early_oth = [flip(t, "c") for t in gu_early]
        out_parts = out_project(attn_in, out_all, heads_cols)
        out_in = exchange(out_parts)
        gu_mid = [after(t, out_parts[0]) for t in (gu_c, gu_d)]
        mid_oth = [flip(t, "c") for t in gu_mid]
        h1 = h0 + sum(t.astype(F32) for t in out_in)

        mn = spread(rms(h1, gains[0]).astype(BF))
        down_got = [after(t, h1) for t in down_got]
        down_oth = [flip(t, "c") for t in down_got]
        gu_e = after(gu_e, *mn, *down_oth)
        gu_e_oth = flip(gu_e, "c")
        gu_own = [*gu_early, *gu_mid, gu_e]
        gu_oth = [*early_oth, *mid_oth, gu_e_oth]
        ff_parts = feed_forward(mn, gu_own, gu_oth, down_got + down_oth, units)
        ff_in = exchange(ff_parts)
        velocity, loss = velocity_and_loss(
            h1, ff_in, gains, head_p, noise.transpose(0, 2, 1), actions.transpose(0, 2, 1)
        )
        velocity = velocity.reshape(own_eps, adim, span).transpose(0, 2, 1)
        return velocity, loss.reshape(own_eps)

    def on_device(*values):
        eps, positions, _ = values[0].shape
        expert = values[8].shape[1]
        fits = (
            (no, ni, nx, nc) == (4, 2, 2, 2)
            and eps == 1
            and values[2].shape[1] <= PAD
            and positions % 256 == 0
            and (expert // (no * nc)) % LANES == 0
            and values[6].shape[0] == 2 * values[10].shape[0] == 2 * values[13].shape[1]
        )
        if not fits:
            return gather_all(*values)
        return fast(*values)

    return on_device


def solution(mesh):
    in_specs = (
        P(("dp", "mp"), None, None),
        P("dp"),
        P("dp", None, None),
        P("dp", None, None),
        P("dp"),
        P(),
        P("dp", None),
        P("dp", None),
        P(),
        P(),
        P("dp", "mp"),
        P("dp", None),
        P("dp", None),
        P("mp", "dp"),
        P(),
        P("dp", "mp"),
        P("dp", "mp"),
        P("mp", "dp"),
        P(),
        P(),
    )
    out_specs = (P(("dp", "mp"), None, None), P(("dp", "mp")))
    ndp, nmp = mesh.shape["dp"], mesh.shape["mp"]
    sizes = (ndp // 2, 2, nmp // 2, 2)
    fine = Mesh(mesh.devices.reshape(sizes), DP + MP)
    names = {"dp": DP, "mp": MP}

    def finer(spec):
        flat = []
        for entry in spec:
            entry = (entry,) if isinstance(entry, str) else entry
            flat.append(None if entry is None else tuple(n for e in entry for n in names[e]))
        return P(*flat)

    return jax.shard_map(
        make(*sizes),
        mesh=fine,
        in_specs=tuple(finer(s) for s in in_specs),
        out_specs=tuple(finer(s) for s in out_specs),
        check_vma=False,
    )
```
